8 devices in a mesh: batch: 1 (over z), col: 2 (over y), row: 4 (over x, core).
Axes of the slice: x: 2, y: 2, z: 1, core: 2. Of those that a mesh axis runs over, the one named last changes fastest.
Arguments:
- pair_rep: bfloat16 [512, 512, 128], P(('batch', 'row'), 'col')
- pair_mask: int32 [512, 512], P(('batch', 'row'), 'col')
- ln_in_gain: bfloat16 [128], replicated
- proj_a: bfloat16 [128, 256], replicated
- gate_a: bfloat16 [128, 256], replicated
- proj_b: bfloat16 [128, 256], replicated
- gate_b: bfloat16 [128, 256], replicated
- gate_out: bfloat16 [128, 128], replicated
- proj_out: bfloat16 [256, 128], replicated
- ln_out_gain: bfloat16 [256], replicated
Outputs:
- output: bfloat16 [512, 512, 128], P(('batch', 'row'), 'col')
All inputs are finite; a program needn't handle non-finite values.
Results may differ from the reference program's by a relative error of at most 0.00477315.
Values are sent between devices in bfloat16 or wider.
A program may use at most 1 GiB of HBM per device.

```python
import math
import jax
import jax.numpy as jnp
from jax import lax

RESIDUES = 512
PAIR_DIM = 128
HIDDEN_DIM = 256

ROW_BLOCK = math.gcd(RESIDUES, 64)
NUM_BLOCKS = RESIDUES // ROW_BLOCK
LN_EPS = 1e-5


def setup_inputs(seed: int = 0, part: int = 0) -> dict:
    part_key = jax.random.fold_in(jax.random.key(seed), part)
    key_pair, key_res, key_drop = jax.random.split(part_key, 3)
    weight_keys = jax.random.split(jax.random.key(seed + 1), 9)

    def normal_matrix(key_w, rows_in, cols_out):
        return (jax.random.normal(key_w, (rows_in, cols_out), jnp.float32) * rows_in ** -0.5).astype(jnp.bfloat16)

    def gain_vector(key_w, vec_len):
        return jax.random.uniform(key_w, (vec_len,), jnp.float32, 0.5, 1.5).astype(jnp.bfloat16)

    pair_rep = jax.random.normal(key_pair, (RESIDUES, RESIDUES, PAIR_DIM), jnp.float32).astype(jnp.bfloat16)
    res_keep = jax.random.randint(key_res, (RESIDUES,), 0, 8) != 0
    pair_keep = jax.random.randint(key_drop, (RESIDUES, RESIDUES), 0, 16) != 0
    pair_mask = (res_keep[:, None] & res_keep[None, :] & pair_keep).astype(jnp.int32)
    return {
        'pair_rep': pair_rep,
        'pair_mask': pair_mask,
        'ln_in_gain': gain_vector(weight_keys[0], PAIR_DIM),
        'proj_a': normal_matrix(weight_keys[1], PAIR_DIM, HIDDEN_DIM),
        'gate_a': normal_matrix(weight_keys[2], PAIR_DIM, HIDDEN_DIM),
        'proj_b': normal_matrix(weight_keys[3], PAIR_DIM, HIDDEN_DIM),
        'gate_b': normal_matrix(weight_keys[4], PAIR_DIM, HIDDEN_DIM),
        'gate_out': normal_matrix(weight_keys[5], PAIR_DIM, PAIR_DIM),
        'proj_out': normal_matrix(weight_keys[6], HIDDEN_DIM, PAIR_DIM),
        'ln_out_gain': gain_vector(weight_keys[7], HIDDEN_DIM),
    }


def layer_norm(values, gain):
    row_mean = jnp.mean(values, axis=-1, keepdims=True)
    centred = values - row_mean
    row_var = jnp.mean(centred * centred, axis=-1, keepdims=True)
    return centred * lax.rsqrt(row_var + LN_EPS) * gain.astype(jnp.float32)


def gated_proj(x_norm, mask_col, proj_w, gate_w):
    proj_val = jnp.dot(x_norm, proj_w, preferred_element_type=jnp.float32)
    gate_val = jax.nn.sigmoid(jnp.dot(x_norm, gate_w, preferred_element_type=jnp.float32))
    return (mask_col * gate_val * proj_val).astype(jnp.bfloat16)


def reference(pair_rep, pair_mask, ln_in_gain, proj_a, gate_a, proj_b, gate_b, gate_out, proj_out, ln_out_gain):
    flat_rows = ROW_BLOCK * RESIDUES
    z_blocks = pair_rep.reshape(NUM_BLOCKS, ROW_BLOCK, RESIDUES, PAIR_DIM)
    m_blocks = pair_mask.reshape(NUM_BLOCKS, ROW_BLOCK, RESIDUES)

    def block_inputs(block_in):
        z_blk, m_blk = block_in
        x_norm = layer_norm(z_blk.astype(jnp.float32), ln_in_gain).astype(jnp.bfloat16).reshape(flat_rows, PAIR_DIM)
        mask_col = m_blk.reshape(flat_rows, 1).astype(jnp.float32)
        return x_norm, mask_col

    def right_block(block_in):
        x_norm, mask_col = block_inputs(block_in)
        return gated_proj(x_norm, mask_col, proj_b, gate_b).astype(jnp.float32).reshape(ROW_BLOCK, RESIDUES, HIDDEN_DIM)

    right = lax.map(right_block, (z_blocks, m_blocks)).reshape(RESIDUES, RESIDUES, HIDDEN_DIM)
    out_w = proj_out.astype(jnp.float32)

    def block_update(block_in):
        x_norm, mask_col = block_inputs(block_in)
        left = gated_proj(x_norm, mask_col, proj_a, gate_a).astype(jnp.float32).reshape(ROW_BLOCK, RESIDUES, HIDDEN_DIM)
        out_gate = jax.nn.sigmoid(jnp.dot(x_norm, gate_out, preferred_element_type=jnp.float32)).reshape(ROW_BLOCK, RESIDUES, PAIR_DIM)
        tri_prod = jnp.einsum('ikc,jkc->ijc', left, right)
        normed = layer_norm(tri_prod, ln_out_gain).astype(jnp.bfloat16).astype(jnp.float32)
        update = jnp.einsum('ijc,cd->ijd', normed, out_w)
        return (block_in[0].astype(jnp.float32) + out_gate * update).astype(jnp.bfloat16)

    return lax.map(block_update, (z_blocks, m_blocks)).reshape(RESIDUES, RESIDUES, PAIR_DIM)
```

```python
import functools

import jax
import jax.numpy as jnp
from jax import lax
from jax.experimental import pallas as pl
from jax.experimental.pallas import tpu as pltpu
from jax.sharding import PartitionSpec as P

LN_EPS = 1e-5

F32 = jnp.float32
BF16 = jnp.bfloat16
VMEM_LIMIT = 60 * 1024 * 1024

ROWS, COLS, PAIR, HID = 128, 256, 128, 256
HALF = ROWS // 2
LANES = 128
FB = 16
CB = 16
IB = 8


def normed(v, gain, scale=None):
    mean = jnp.mean(v, axis=-1, keepdims=True)
    cen = v - mean
    var = jnp.mean(cen * cen, axis=-1, keepdims=True)
    rs = lax.rsqrt(var + LN_EPS)
    if scale is not None:
        rs = rs * scale
    return (cen * rs * gain).astype(BF16)


def ln_kernel(z_ref, m_ref, g_ref, o_ref):
    gain = g_ref[...]
    for r in range(FB):
        o_ref[r] = normed(z_ref[r].astype(F32), gain, m_ref[0, :, r:r + 1])


def masked_norm(z_tile, mask_t, gain, half):
    steps = HALF // FB
    return pl.pallas_call(
        ln_kernel,
        grid=(steps,),
        out_shape=jax.ShapeDtypeStruct((HALF, COLS, PAIR), BF16),
        in_specs=[
            pl.BlockSpec((FB, COLS, PAIR), lambda s: (half * steps + s, 0, 0)),
            pl.BlockSpec((1, COLS, FB), lambda s: (half * steps + s, 0, 0)),
            pl.BlockSpec((1, PAIR), lambda s: (0, 0)),
        ],
        out_specs=pl.BlockSpec((FB, COLS, PAIR), lambda s: (s, 0, 0)),
        compiler_params=pltpu.CompilerParams(vmem_limit_bytes=VMEM_LIMIT),
        cost_estimate=pl.CostEstimate(flops=10**9, bytes_accessed=2 * HALF * COLS * PAIR * 2, transcendentals=0),
        name='masked_norm',
    )(z_tile, mask_t, gain)


def project_block(read_row, w_ref, o_ref, scr):
    def one_row(r, _):
        both = lax.dot_general(w_ref[...], read_row(r), (((1,), (1,)), ((), ())), preferred_element_type=F32)
        proj = both[:HID]
        val = proj + jnp.tanh(both[HID:]) * proj
        for n in range(COLS // LANES):
            scr[n, pl.ds(r, HID, stride=FB), :] = val[:, n * LANES:(n + 1) * LANES]
        return 0

    lax.fori_loop(0, FB, one_row, 0, unroll=4)
    for n in range(COLS // LANES):
        o_ref[:, :, n * LANES:(n + 1) * LANES] = scr[n].reshape(HID, FB, LANES).astype(BF16)


def front_one_kernel(x_ref, w_ref, o_ref, scr):
    project_block(lambda r: x_ref[r], w_ref, o_ref, scr)


def front_cost(rows):
    return pl.CostEstimate(flops=rows * COLS * PAIR * HID * 4 * 2, bytes_accessed=rows * COLS * (PAIR + HID) * 2,
                           transcendentals=rows * COLS * HID)


def front_one(x_half, w_t):
    return pl.pallas_call(
        front_one_kernel,
        grid=(HALF // FB,),
        out_shape=jax.ShapeDtypeStruct((HID, HALF, COLS), BF16),
        in_specs=[
            pl.BlockSpec((FB, COLS, PAIR), lambda s: (s, 0, 0)),
            pl.BlockSpec((2 * HID, PAIR), lambda s: (0, 0)),
        ],
        out_specs=pl.BlockSpec((HID, FB, COLS), lambda s: (0, s, 0)),
        scratch_shapes=[pltpu.VMEM((COLS // LANES, HID * FB, LANES), F32)],
        compiler_params=pltpu.CompilerParams(vmem_limit_bytes=VMEM_LIMIT),
        cost_estimate=front_cost(HALF),
        name='front_a',
    )(x_half, w_t)


def front_pair_kernel(sel, own_d, own_o, sib_d, sib_o, w_ref, o_ref, x_scr, scr):
    side = pl.program_id(0)
    diag = sel[1]
    for want_side, want_diag, ref in ((0, 1, own_d), (0, 0, own_o), (1, 1, sib_d), (1, 0, sib_o)):
        @pl.when((side == want_side) & (diag == want_diag))
        def _(ref=ref):
            x_scr[...] = ref[...]
    project_block(lambda r: x_scr[r], w_ref, o_ref, scr)


def front_pair(sel, own_d, own_o, sib_d, sib_o, w_t):
    steps = HALF // FB

    def source(want_side, want_diag):
        def index(side, s, sel):
            if want_side == 0:
                here = jnp.where(side == 0, s, steps - 1)
            else:
                here = jnp.where(side == 1, s, 0)
            return (jnp.where(sel[1] == want_diag, here, 0), 0, 0)
        return pl.BlockSpec((FB, COLS, PAIR), index)

    return pl.pallas_call(
        front_pair_kernel,
        grid_spec=pltpu.PrefetchScalarGridSpec(
            num_scalar_prefetch=1,
            grid=(2, steps),
            in_specs=[source(0, 1), source(0, 0), source(1, 1), source(1, 0),
                      pl.BlockSpec((2 * HID, PAIR), lambda side, s, sel: (0, 0))],
            out_specs=pl.BlockSpec((HID, FB, COLS), lambda side, s, sel: (0, (side ^ sel[0]) * steps + s, 0)),
            scratch_shapes=[pltpu.VMEM((FB, COLS, PAIR), BF16), pltpu.VMEM((COLS // LANES, HID * FB, LANES), F32)],
        ),
        out_shape=jax.ShapeDtypeStruct((HID, 2 * HALF, COLS), BF16),
        compiler_params=pltpu.CompilerParams(vmem_limit_bytes=VMEM_LIMIT),
        cost_estimate=front_cost(2 * HALF),
        name='front_b',
    )(sel, own_d, own_o, sib_d, sib_o, w_t)


def back_kernel(a00, a01, a10, a11, b0, b1, z_ref, gin_ref, gate_ref, gout_ref, proj_ref, *rest):
    o_ref, o_scr = rest[-2:]
    step = pl.program_id(0)
    n_c = HID // CB

    @pl.when(step < n_c)
    def _():
        for c in range(CB):
            lhs0 = jnp.concatenate([a00[c], a10[c]], axis=0)
            lhs1 = jnp.concatenate([a01[c], a11[c]], axis=0)
            dims = (((1,), (1,)), ((), ()))
            acc = lax.dot_general(lhs0, b0[c], dims, preferred_element_type=F32)
            acc = acc + lax.dot_general(lhs1, b1[c], dims, preferred_element_type=F32)
            base = pl.multiple_of((step * CB + c) * ROWS, ROWS)
            o_scr[pl.ds(base, ROWS), :] = acc

    @pl.when(step >= n_c)
    def _():
        first = (step - n_c) * IB
        gain_out = gout_ref[...]

        def one_row(i, _):
            tri = o_scr[pl.ds(first + i, HID, stride=ROWS), :]
            mean = jnp.mean(tri, axis=0, keepdims=True)
            cen = tri - mean
            var = jnp.mean(cen * cen, axis=0, keepdims=True)
            y = (cen * lax.rsqrt(var + LN_EPS) * gain_out).astype(BF16)
            u = lax.dot_general(y, proj_ref[...], (((0,), (0,)), ((), ())), preferred_element_type=F32)
            z = z_ref[i].reshape(2 * HALF, PAIR).astype(F32)
            x = normed(z, gin_ref[...])
            g = jax.nn.sigmoid(jnp.dot(x, gate_ref[...], preferred_element_type=F32))
            o_ref[i] = (z + g * u).astype(BF16).reshape(2, HALF, PAIR)
            return 0

        lax.fori_loop(0, IB, one_row, 0, unroll=2)


def back(a_parts, b_parts, z_tile, gain_in, gate_out, gain_out, proj_out, half, prev):
    n_c, n_i = HID // CB, ROWS // IB
    z4 = z_tile.reshape(ROWS, 2, 2 * HALF, PAIR)

    def chan(rows):
        return pl.BlockSpec((CB, rows, COLS), lambda s: (jnp.minimum(s, n_c - 1), 0, 0))

    tile = pl.BlockSpec((IB, 2, HALF, PAIR), lambda s: (jnp.maximum(s - n_c, 0), 0, half, 0))

    def whole(*shape):
        return pl.BlockSpec(shape, lambda s: (0,) * len(shape))

    args = [*a_parts, *b_parts, z4, gain_in, gate_out, gain_out, proj_out]
    specs = [chan(HALF)] * 4 + [chan(2 * HALF)] * 2 + [tile, whole(1, PAIR), whole(PAIR, PAIR), whole(HID, 1), whole(HID, PAIR)]
    aliases = {}
    if prev is not None:
        aliases = {len(args): 0}
        args.append(prev)
        specs.append(pl.BlockSpec(memory_space=pl.ANY))
    return pl.pallas_call(
        back_kernel,
        grid=(n_c + n_i,),
        out_shape=jax.ShapeDtypeStruct((ROWS, 2, 2 * HALF, PAIR), BF16),
        in_specs=specs,
        out_specs=tile,
        scratch_shapes=[pltpu.VMEM((HID * ROWS, 2 * HALF), F32)],
        input_output_aliases=aliases,
        compiler_params=pltpu.CompilerParams(vmem_limit_bytes=VMEM_LIMIT),
        cost_estimate=pl.CostEstimate(flops=HID * ROWS * ROWS * 512 * 2 * 4, bytes_accessed=64 * 2**20, transcendentals=0),
        name='back',
    )(*args)


def solution(mesh):
    tile_spec = P(('batch', 'row'), 'col', None)
    mask_spec = P(('batch', 'row'), 'col')
    repl_spec = P()
    axes = ('col', 'row')
    two = range(2)

    def dev(chip_x, core, chip_y):
        return chip_y * 4 + chip_x * 2 + core

    everyone = [(x, c, y) for x in two for c in two for y in two]
    pairs_y = [(dev(x, c, y), dev(x, c, 1 - y)) for x, c, y in everyone]
    pairs_x = [(dev(x, c, y), dev(1 - x, c, y)) for x, c, y in everyone if x == y]
    pairs_xy = [(dev(x, c, y), dev(1 - x, c, 1 - y)) for x, c, y in everyone if x != y]
    sib_diag = [(dev(x, c, y), dev(x, 1 - c, y)) for x, c, y in everyone if x == y]
    sib_off = [(dev(x, c, y), dev(x, 1 - c, y)) for x, c, y in everyone if x != y]

    def send(v, pairs):
        return lax.ppermute(v, axes, pairs)

    def after(v, *others):
        return lax.optimization_barrier((v, *others))[0]

    def per_device(z_tile, mask_tile, ln_in_gain, proj_a, gate_a, proj_b, gate_b, gate_out, proj_out, ln_out_gain):
        row, col = lax.axis_index('row'), lax.axis_index('col')
        sel = jnp.stack([row % 2, (row // 2 == col).astype(jnp.int32)]).astype(jnp.int32)
        mask_t = mask_tile.astype(F32).reshape(ROWS // FB, FB, COLS).transpose(0, 2, 1)
        gain_in = ln_in_gain.astype(F32).reshape(1, PAIR)
        gain_out = ln_out_gain.astype(F32).reshape(HID, 1)
        w_a = (jnp.concatenate([proj_a, gate_a], axis=1) * 0.5).T
        w_b = (jnp.concatenate([proj_b, gate_b], axis=1) * 0.5).T

        x0 = masked_norm(z_tile, mask_t, gain_in, 0)
        x1 = masked_norm(z_tile, mask_t, gain_in, 1)
        y0 = send(x0, pairs_y)
        y1 = send(x1, pairs_y)
        p0 = send(x0, pairs_x)
        q0 = send(y0, pairs_x)
        p1 = send(after(x1, y0), pairs_x)
        q1 = send(after(x1, y1), pairs_xy)
        a00, a10 = front_one(x0, w_a), front_one(x1, w_a)
        b00 = front_pair(sel, x0, p0, send(x0, sib_diag), send(p0, sib_off), w_b)
        a01 = front_one(y0, w_a)
        b01 = front_pair(sel, y0, q0, send(y0, sib_diag), send(q0, sib_off), w_b)
        a11 = front_one(y1, w_a)
        a_parts = [a00, a01, a10, a11]
        rest = (z_tile, gain_in, gate_out, gain_out, proj_out)
        out = back(a_parts, [b00, b01], *rest, 0, None)
        b10 = front_pair(sel, x1, p1, send(x1, sib_diag), send(p1, sib_off), w_b)
        b11 = front_pair(sel, y1, q1, send(y1, sib_diag), send(q1, sib_off), w_b)
        out = back(a_parts, [b10, b11], *rest, 1, out)
        return out.reshape(ROWS, COLS, PAIR)

    return jax.shard_map(per_device, mesh=mesh, in_specs=(tile_spec, mask_spec) + (repl_spec,) * 8, out_specs=tile_spec, check_vma=False)
```

```python
import functools

import jax
import jax.numpy as jnp
from jax import lax
from jax.experimental import pallas as pl
from jax.experimental.pallas import tpu as pltpu
from jax.sharding import PartitionSpec as P

LN_EPS = 1e-5

F32 = jnp.float32
BF16 = jnp.bfloat16
VMEM_LIMIT = 60 * 1024 * 1024

ROWS, COLS, PAIR, HID = 128, 256, 128, 256
HALF = ROWS // 2
LANES = 128
PITCH = HID + 8
OPITCH = ROWS + 8
CH = 128
FB = 16
CB = 16
IB = 8


def normed_t(v, gain):
    mean = jnp.mean(v, axis=0, keepdims=True)
    cen = v - mean
    var = jnp.mean(cen * cen, axis=0, keepdims=True)
    return cen * lax.rsqrt(var + LN_EPS) * gain


def ln_kernel(z_ref, m_ref, g_ref, *rest):
    x_ref, xm_ref = rest[-2:]
    gain = g_ref[...]
    for r in range(FB):
        z = z_ref[r].reshape(2, 2, HALF, PAIR)
        z = jnp.concatenate([z[0, 0], z[1, 0], z[0, 1], z[1, 1]], axis=0)
        x = normed_t(z.astype(F32).T, gain)
        x_ref[r] = x.astype(BF16)
        xm_ref[r] = (x * m_ref[r:r + 1, :].astype(F32)).astype(BF16)


def masked_norm(z_tile, mask, gain, half, prev):
    steps = HALF // FB
    args = [z_tile, mask, gain]
    in_specs = [
        pl.BlockSpec((FB, COLS, PAIR), lambda s: (half * steps + s, 0, 0)),
        pl.BlockSpec((FB, COLS), lambda s: (half * steps + s, 0)),
        pl.BlockSpec((PAIR, 1), lambda s: (0, 0)),
    ]
    aliases = {}
    if prev is not None:
        aliases = {len(args): 0}
        args.append(prev)
        in_specs.append(pl.BlockSpec(memory_space=pl.ANY))
    return pl.pallas_call(
        ln_kernel,
        grid=(steps,),
        out_shape=(jax.ShapeDtypeStruct((ROWS, PAIR, COLS), BF16), jax.ShapeDtypeStruct((HALF, PAIR, COLS), BF16)),
        in_specs=in_specs,
        out_specs=(pl.BlockSpec((FB, PAIR, COLS), lambda s: (half * steps + s, 0, 0)),
                   pl.BlockSpec((FB, PAIR, COLS), lambda s: (s, 0, 0))),
        input_output_aliases=aliases,
        compiler_params=pltpu.CompilerParams(vmem_limit_bytes=VMEM_LIMIT),
        cost_estimate=pl.CostEstimate(flops=10**9, bytes_accessed=3 * HALF * COLS * PAIR * 2, transcendentals=0),
        name='masked_norm',
    )(*args)


def project_block(read_row, w_ref, o_ref, scr):
    for r in range(FB):
        x = read_row(r)
        for c in range(0, HID, CH):
            both = jnp.dot(w_ref[2 * c:2 * (c + CH), :], x, preferred_element_type=F32)
            proj = both[:CH]
            val = proj + jnp.tanh(both[CH:]) * proj
            for n in range(COLS // LANES):
                scr[n, pl.ds(r * PITCH + c, CH), :] = val[:, n * LANES:(n + 1) * LANES]

    def channel(c, _):
        for n in range(COLS // LANES):
            o_ref[c, :, n * LANES:(n + 1) * LANES] = scr[n, pl.ds(c, FB, stride=PITCH), :].astype(BF16)
        return 0

    lax.fori_loop(0, HID, channel, 0, unroll=16)


def front_one_kernel(x_ref, w_ref, o_ref, scr):
    project_block(lambda r: x_ref[r], w_ref, o_ref, scr)


def front_cost(rows):
    return pl.CostEstimate(flops=rows * COLS * PAIR * HID * 4 * 2, bytes_accessed=rows * COLS * (PAIR + HID) * 2,
                           transcendentals=rows * COLS * HID)


def front_one(x_half, w_t):
    return pl.pallas_call(
        front_one_kernel,
        grid=(HALF // FB,),
        out_shape=jax.ShapeDtypeStruct((HID, HALF, COLS), BF16),
        in_specs=[
            pl.BlockSpec((FB, PAIR, COLS), lambda s: (s, 0, 0)),
            pl.BlockSpec((2 * HID, PAIR), lambda s: (0, 0)),
        ],
        out_specs=pl.BlockSpec((HID, FB, COLS), lambda s: (0, s, 0)),
        scratch_shapes=[pltpu.VMEM((COLS // LANES, FB * PITCH, LANES), F32)],
        compiler_params=pltpu.CompilerParams(vmem_limit_bytes=VMEM_LIMIT),
        cost_estimate=front_cost(HALF),
        name='front_a',
    )(x_half, w_t)


def front_pair_kernel(sel, own_d, own_o, sib_d, sib_o, w_ref, o_ref, x_scr, scr):
    side = pl.program_id(0)
    diag = sel[1]
    for want_side, want_diag, ref in ((0, 1, own_d), (0, 0, own_o), (1, 1, sib_d), (1, 0, sib_o)):
        @pl.when((side == want_side) & (diag == want_diag))
        def _(ref=ref):
            x_scr[...] = ref[...]
    project_block(lambda r: x_scr[r], w_ref, o_ref, scr)


def front_pair(sel, own_d, own_o, sib_d, sib_o, w_t):
    steps = HALF // FB

    def source(want_side, want_diag):
        def index(side, s, sel):
            if want_side == 0:
                here = jnp.where(side == 0, s, steps - 1)
            else:
                here = jnp.where(side == 1, s, 0)
            return (jnp.where(sel[1] == want_diag, here, 0), 0, 0)
        return pl.BlockSpec((FB, PAIR, COLS), index)

    return pl.pallas_call(
        front_pair_kernel,
        grid_spec=pltpu.PrefetchScalarGridSpec(
            num_scalar_prefetch=1,
            grid=(2, steps),
            in_specs=[source(0, 1), source(0, 0), source(1, 1), source(1, 0),
                      pl.BlockSpec((2 * HID, PAIR), lambda side, s, sel: (0, 0))],
            out_specs=pl.BlockSpec((HID, FB, COLS), lambda side, s, sel: (0, (side ^ sel[0]) * steps + s, 0)),
            scratch_shapes=[pltpu.VMEM((FB, PAIR, COLS), BF16), pltpu.VMEM((COLS // LANES, FB * PITCH, LANES), F32)],
        ),
        out_shape=jax.ShapeDtypeStruct((HID, 2 * HALF, COLS), BF16),
        compiler_params=pltpu.CompilerParams(vmem_limit_bytes=VMEM_LIMIT),
        cost_estimate=front_cost(2 * HALF),
        name='front_b',
    )(sel, own_d, own_o, sib_d, sib_o, w_t)


def back_kernel(a00, a01, a10, a11, b0, b1, z_ref, x_ref, gate_ref, gout_ref, proj_ref, *rest):
    o_ref, o_scr = rest[-2:]
    step = pl.program_id(0)
    n_c = HID // CB

    @pl.when(step < n_c)
    def _():
        for c in range(CB):
            lhs0 = jnp.concatenate([a00[c], a10[c]], axis=0)
            lhs1 = jnp.concatenate([a01[c], a11[c]], axis=0)
            dims = (((1,), (1,)), ((), ()))
            acc = lax.dot_general(lhs0, b0[c], dims, preferred_element_type=F32)
            acc = acc + lax.dot_general(lhs1, b1[c], dims, preferred_element_type=F32)
            o_scr[pl.ds(pl.multiple_of((step * CB + c) * OPITCH, 8), ROWS), :] = acc

    @pl.when(step >= n_c)
    def _():
        first = (step - n_c) * IB
        gain_out = gout_ref[...]

        def one_row(i, _):
            tri = o_scr[pl.ds(first + i, HID, stride=OPITCH), :]
            y = normed_t(tri, gain_out).astype(BF16)
            u = jnp.dot(proj_ref[...], y, preferred_element_type=F32)
            g = jax.nn.sigmoid(jnp.dot(gate_ref[...], x_ref[i], preferred_element_type=F32))
            z = z_ref[i].reshape(2 * HALF, PAIR).astype(F32)
            o_ref[i] = (z + (g * u).T).astype(BF16).reshape(2, HALF, PAIR)
            return 0

        lax.fori_loop(0, IB, one_row, 0, unroll=4)


def back(a_parts, b_parts, z_tile, x_tile, gate_out, gain_out, proj_out, half, prev):
    n_c, n_i = HID // CB, ROWS // IB
    z4 = z_tile.reshape(ROWS, 2, 2 * HALF, PAIR)

    def chan(rows):
        return pl.BlockSpec((CB, rows, COLS), lambda s: (jnp.minimum(s, n_c - 1), 0, 0))

    tile = pl.BlockSpec((IB, 2, HALF, PAIR), lambda s: (jnp.maximum(s - n_c, 0), 0, half, 0))

    x_spec = pl.BlockSpec((IB, PAIR, 2 * HALF), lambda s: (jnp.maximum(s - n_c, 0), 0, half))

    def whole(*shape):
        return pl.BlockSpec(shape, lambda s: (0,) * len(shape))

    args = [*a_parts, *b_parts, z4, x_tile, gate_out, gain_out, proj_out]
    specs = [chan(HALF)] * 4 + [chan(2 * HALF)] * 2 + [tile, x_spec, whole(PAIR, PAIR), whole(HID, 1), whole(PAIR, HID)]
    aliases = {}
    if prev is not None:
        aliases = {len(args): 0}
        args.append(prev)
        specs.append(pl.BlockSpec(memory_space=pl.ANY))
    return pl.pallas_call(
        back_kernel,
        grid=(n_c + n_i,),
        out_shape=jax.ShapeDtypeStruct((ROWS, 2, 2 * HALF, PAIR), BF16),
        in_specs=specs,
        out_specs=tile,
        scratch_shapes=[pltpu.VMEM((HID * OPITCH, 2 * HALF), F32)],
        input_output_aliases=aliases,
        compiler_params=pltpu.CompilerParams(vmem_limit_bytes=VMEM_LIMIT),
        cost_estimate=pl.CostEstimate(flops=HID * ROWS * ROWS * 512 * 2 * 4, bytes_accessed=64 * 2**20, transcendentals=0),
        name='back',
    )(*args)


def solution(mesh):
    tile_spec = P(('batch', 'row'), 'col', None)
    mask_spec = P(('batch', 'row'), 'col')
    repl_spec = P()
    axes = ('col', 'row')
    two = range(2)

    def dev(chip_x, core, chip_y):
        return chip_y * 4 + chip_x * 2 + core

    everyone = [(x, c, y) for x in two for c in two for y in two]
    pairs_y = [(dev(x, c, y), dev(x, c, 1 - y)) for x, c, y in everyone]
    pairs_x = [(dev(x, c, y), dev(1 - x, c, y)) for x, c, y in everyone if x == y]
    pairs_xy = [(dev(x, c, y), dev(1 - x, c, 1 - y)) for x, c, y in everyone if x != y]
    sib_diag = [(dev(x, c, y), dev(x, 1 - c, y)) for x, c, y in everyone if x == y]
    sib_off = [(dev(x, c, y), dev(x, 1 - c, y)) for x, c, y in everyone if x != y]

    def send(v, pairs):
        return lax.ppermute(v, axes, pairs)

    def after(v, *others):
        return lax.optimization_barrier((v, *others))[0]

    def per_device(z_tile, mask_tile, ln_in_gain, proj_a, gate_a, proj_b, gate_b, gate_out, proj_out, ln_out_gain):
        row, col = lax.axis_index('row'), lax.axis_index('col')
        sel = jnp.stack([row % 2, (row // 2 == col).astype(jnp.int32)]).astype(jnp.int32)
        mask_t = mask_tile.reshape(ROWS, 2, 2, HALF).transpose(0, 2, 1, 3).reshape(ROWS, COLS)
        gain_in = ln_in_gain.astype(F32).reshape(PAIR, 1)
        gain_out = ln_out_gain.astype(F32).reshape(HID, 1)

        def weights(proj, gate):
            both = jnp.stack([proj.T.reshape(HID // CH, CH, PAIR), gate.T.reshape(HID // CH, CH, PAIR)], axis=1)
            return both.reshape(2 * HID, PAIR) * 0.5

        w_a, w_b = weights(proj_a, gate_a), weights(proj_b, gate_b)

        x_tile, x0 = masked_norm(z_tile, mask_t, gain_in, 0, None)
        x_tile, x1 = masked_norm(z_tile, mask_t, gain_in, 1, x_tile)
        y0 = send(x0, pairs_y)
        p0 = send(x0, pairs_x)
        sx0, sx1 = send(x0, sib_diag), send(x1, sib_diag)
        y1 = send(x1, pairs_y)
        a00, a10 = front_one(x0, w_a), front_one(x1, w_a)
        y0, p0, _, _ = lax.optimization_barrier((y0, p0, a00, a10))
        q0 = send(y0, pairs_x)
        p1 = send(after(x1, y0), pairs_x)
        sp0, sy0 = send(p0, sib_off), send(y0, sib_diag)
        a01 = front_one(y0, w_a)
        b00 = front_pair(sel, x0, p0, sx0, sp0, w_b)
        y1, q0, _, _ = lax.optimization_barrier((y1, q0, a01, b00))
        q1 = send(after(x1, y1), pairs_xy)
        sq0, sy1 = send(q0, sib_off), send(y1, sib_diag)
        a11 = front_one(y1, w_a)
        b01 = front_pair(sel, y0, q0, sy0, sq0, w_b)
        a_parts = [a00, a01, a10, a11]
        rest = (z_tile, x_tile, gate_out.T, gain_out, proj_out.T)
        out = back(a_parts, [b00, b01], *rest, 0, None)
        p1, q1, _ = lax.optimization_barrier((p1, q1, out))
        b10 = front_pair(sel, x1, p1, sx1, send(p1, sib_off), w_b)
        b11 = front_pair(sel, y1, q1, sy1, send(q1, sib_off), w_b)
        out = back(a_parts, [b10, b11], *rest, 1, out)
        return out.reshape(ROWS, COLS, PAIR)

    return jax.shard_map(per_device, mesh=mesh, in_specs=(tile_spec, mask_spec) + (repl_spec,) * 8, out_specs=tile_spec, check_vma=False)
```

```python
import jax
import jax.numpy as jnp
from jax import lax
from jax.experimental import pallas as pl
from jax.experimental.pallas import tpu as pltpu
from jax.sharding import PartitionSpec as P

LN_EPS = 1e-5
F32 = jnp.float32
BF16 = jnp.bfloat16
VMEM_LIMIT = 60 * 1024 * 1024
MESH = pl.DeviceIdType.MESH

ROWS, COLS, PAIR, HID = 128, 256, 128, 256
HALF = ROWS // 2
LANES = 128
FB = 16
NCH = ROWS // FB
NH = NCH // 2
CH = 128
PITCH = HID + 8
OPITCH = ROWS + 8
CB = 16
IB = 8
N_C, N_I = HID // CB, ROWS // IB


def normed_t(v, gain):
    mean = jnp.mean(v, axis=0, keepdims=True)
    cen = v - mean
    var = jnp.mean(cen * cen, axis=0, keepdims=True)
    return cen * lax.rsqrt(var + LN_EPS) * gain


def norm_chunk(z_ref, m_ref, first, gain, x_ref, xm_ref):
    for r in range(FB):
        z = z_ref[r].reshape(2, 2, HALF, PAIR)
        z = jnp.concatenate([z[0, 0], z[1, 0], z[0, 1], z[1, 1]], axis=0)
        x = normed_t(z.astype(F32).T, gain)
        x_ref[r] = x.astype(BF16)
        xm_ref[r] = (x * m_ref[pl.ds(first + r, 1), :].astype(F32)).astype(BF16)


def project_chunk(x_ref, w_ref, o_ref, scr):
    for r in range(FB):
        x = x_ref[r]
        for c in range(0, HID, CH):
            both = jnp.dot(w_ref[2 * c:2 * (c + CH), :], x, preferred_element_type=F32)
            proj = both[:CH]
            val = proj + jnp.tanh(both[CH:]) * proj
            for n in range(COLS // LANES):
                scr[n, pl.ds(r * PITCH + c, CH), :] = val[:, n * LANES:(n + 1) * LANES]

    def channel(c, _):
        for n in range(COLS // LANES):
            o_ref[c, :, n * LANES:(n + 1) * LANES] = scr[n, pl.ds(c, FB, stride=PITCH), :].astype(BF16)
        return 0

    lax.fori_loop(0, HID, channel, 0, unroll=16)


def back_body(step, a0, a1, b0, b1, z_ref, x_ref, o_ref, gate_ref, gain_ref, proj_ref, o_scr):
    @pl.when(step < N_C)
    def _():
        for c in range(CB):
            dims = (((1,), (1,)), ((), ()))
            acc = lax.dot_general(a0[0, c], b0[0, c], dims, preferred_element_type=F32)
            acc = acc + lax.dot_general(a1[0, c], b1[0, c], dims, preferred_element_type=F32)
            o_scr[pl.ds(pl.multiple_of((step * CB + c) * OPITCH, 8), ROWS), :] = acc

    @pl.when(step >= N_C)
    def _():
        first = (step - N_C) * IB
        gain = gain_ref[...]

        def one_row(i, _):
            tri = o_scr[pl.ds(first + i, HID, stride=OPITCH), :]
            y = normed_t(tri, gain).astype(BF16)
            u = jnp.dot(proj_ref[...], y, preferred_element_type=F32)
            g = jax.nn.sigmoid(jnp.dot(gate_ref[...], x_ref[i], preferred_element_type=F32))
            z = z_ref[i].reshape(2 * HALF, PAIR).astype(F32)
            o_ref[i] = (z + (g * u).T).astype(BF16).reshape(2, HALF, PAIR)
            return 0

        lax.fori_loop(0, IB, one_row, 0, unroll=4)


def back_specs(half):
    def chan(slot):
        return pl.BlockSpec((1, CB, ROWS, COLS), lambda s: (slot, jnp.minimum(s, N_C - 1), 0, 0))

    tile = pl.BlockSpec((IB, 2, HALF, PAIR), lambda s: (jnp.maximum(s - N_C, 0), 0, half, 0))
    x_spec = pl.BlockSpec((IB, PAIR, 2 * HALF), lambda s: (jnp.maximum(s - N_C, 0), 0, half))
    return [chan(0), chan(1), chan(2 + 2 * half), chan(3 + 2 * half), tile, x_spec], tile


def main_kernel(z_ref, z4_ref, mask_ref, gain_ref, w_ref, gate_ref, gout_ref, proj_ref,
                xb, g_ref, xt, out_ref,
                zbuf, xubuf, xmbuf, xin, obuf, scr, o_scr,
                zsem, xusem, xmsem, xsem, osem,
                y_s, p_s, q_s, s0_s, s1_s, y_r, p_r, q_r, s0_r, s1_r):
    row, col = lax.axis_index('row'), lax.axis_index('col')
    chip, core = row // 2, row % 2
    ydev = {'col': 1 - col}
    xdev = {'row': (1 - chip) * 2 + core}
    xydev = {'row': (1 - chip) * 2 + core, 'col': 1 - col}
    sdev = {'row': chip * 2 + 1 - core}
    diag = chip == col
    off = chip != col
    mine = 1 - diag.astype(jnp.int32)

    def part(k, slot, ch):
        return xb.at[k, slot, pl.ds(ch * FB, FB)]

    def rdma(src, dst, send, recv, dev):
        return pltpu.make_async_remote_copy(src_ref=src, dst_ref=dst, send_sem=send, recv_sem=recv,
                                            device_id=dev, device_id_type=MESH)

    def y(ch):
        return rdma(part(0, 0, ch), part(1, 0, ch), y_s.at[ch], y_r.at[ch], ydev)

    def p(ch):
        return rdma(part(0, 0, ch), part(0, 1, ch), p_s.at[ch], p_r.at[ch], xdev)

    def q_relay(ch):
        return rdma(part(1, 0, ch), part(1, 1, ch), q_s.at[ch], q_r.at[ch], xdev)

    def q_direct(ch):
        return rdma(part(0, 0, ch), part(1, 1, ch), q_s.at[ch], q_r.at[ch], xydev)

    def s0(ch):
        return rdma(part(0, mine, ch), part(0, 2, ch), s0_s.at[ch], s0_r.at[ch], sdev)

    def s1(ch):
        return rdma(part(1, mine, ch), part(1, 2, ch), s1_s.at[ch], s1_r.at[ch], sdev)

    barrier = pltpu.get_barrier_semaphore()
    for dev in (ydev, xdev, xydev, sdev):
        pl.semaphore_signal(barrier, inc=1, device_id=dev, device_id_type=MESH)

    def zload(ch):
        return pltpu.make_async_copy(z_ref.at[pl.ds(ch * FB, FB)], zbuf.at[ch % 2], zsem.at[ch % 2])

    def xustore(ch):
        return pltpu.make_async_copy(xubuf.at[ch % 2], xt.at[pl.ds(ch * FB, FB)], xusem.at[ch % 2])

    def xmstore(ch):
        return pltpu.make_async_copy(xmbuf.at[ch % 2], part(0, 0, ch), xmsem.at[ch % 2])

    def publish(ch):
        xmstore(ch).wait()
        y(ch).start()

        @pl.when(diag)
        def _():
            s0(ch).start()

        @pl.when(diag & (ch < NH))
        def _():
            p(ch).start()

    gain = gain_ref[...]
    zload(0).start()
    pl.semaphore_wait(barrier, 4)

    def norm_step(ch, _):
        @pl.when(ch + 1 < NCH)
        def _():
            zload(ch + 1).start()

        @pl.when(ch >= 2)
        def _():
            xustore(ch - 2).wait()

        zload(ch).wait()
        norm_chunk(zbuf.at[ch % 2], mask_ref, ch * FB, gain, xubuf.at[ch % 2], xmbuf.at[ch % 2])
        xustore(ch).start()
        xmstore(ch).start()

        @pl.when(ch >= 1)
        def _():
            publish(ch - 1)
        return 0

    lax.fori_loop(0, NCH, norm_step, 0)
    publish(NCH - 1)
    xustore(NCH - 2).wait()
    xustore(NCH - 1).wait()

    def xload(k, slot, ch, t):
        return pltpu.make_async_copy(part(k, slot, ch), xin.at[t], xsem.at[t])

    def ostore(dst, block, t):
        return pltpu.make_async_copy(obuf.at[t % 2], g_ref.at[dst, :, pl.ds(block * FB, FB), :], osem.at[t % 2])

    def project(first_use, t, weight, dst, block):
        @pl.when(jnp.logical_not(first_use))
        def _():
            ostore(0, 0, t).wait()
        project_chunk(xin.at[t], w_ref.at[weight], obuf.at[t % 2], scr)
        ostore(dst, block, t).start()

    def window1(i, _):
        k, ch = i // NH, i % NH
        y(i).wait_recv()

        @pl.when(diag)
        def _():
            s1(i).start()

        @pl.when(diag & (i < NH))
        def _():
            q_relay(i).start()

        @pl.when(diag & (i == NH - 1))
        def _():
            for c in range(NH, NCH):
                p(c).start()

        @pl.when(off & (i == NCH - 2))
        def _():
            for c in range(NH, NCH):
                q_direct(c).start()

        @pl.when(off & (i < NH))
        def _():
            p(ch).wait_recv()
            s0(ch).start()

        @pl.when(off & (i >= NH))
        def _():
            q_relay(ch).wait_recv()
            s1(ch).start()

        xload(0, 0, i, 0).start()
        xload(1, 0, i, 1).start()
        xload(k, mine, ch, 2).start()

        def step(t, _):
            @pl.when((t == 1) & (i < NH))
            def _():
                s0(ch).wait_recv()

            @pl.when((t == 1) & (i >= NH))
            def _():
                s1(ch).wait_recv()

            @pl.when(t == 1)
            def _():
                xload(k, 2, ch, 3).start()

            xload(0, 0, 0, t).wait()
            is_b = t // 2
            own_block = jnp.where(t == 2, core, 1 - core) * NH + ch
            project((i == 0) & (t < 2), t, is_b, jnp.where(is_b == 1, 2 + k, t), jnp.where(is_b == 1, own_block, i))
            return 0

        lax.fori_loop(0, 4, step, 0)
        return 0

    lax.fori_loop(0, NCH, window1, 0)
    ostore(0, 0, 0).wait()
    ostore(0, 0, 1).wait()

    specs, out_spec = back_specs(0)

    def pipe(a0, a1, b0, b1, zr, xr, o):
        back_body(pl.program_id(0), a0, a1, b0, b1, zr, xr, o, gate_ref, gout_ref, proj_ref, o_scr)

    pltpu.emit_pipeline(pipe, grid=(N_C + N_I,), in_specs=specs, out_specs=[out_spec])(
        g_ref, g_ref, g_ref, g_ref, z4_ref, xt, out_ref)

    def window2(i, _):
        ch = NH + i

        @pl.when(off)
        def _():
            p(ch).wait_recv()
            s0(ch).start()
            q_direct(ch).wait_recv()
            s1(ch).start()

        xload(0, mine, ch, 0).start()
        xload(1, mine, ch, 1).start()

        def step(t, _):
            @pl.when(t == 1)
            def _():
                s0(ch).wait_recv()
                xload(0, 2, ch, 2).start()
                s1(ch).wait_recv()
                xload(1, 2, ch, 3).start()

            xload(0, 0, 0, t).wait()
            project((i == 0) & (t < 2), t, 1, 4 + t % 2, jnp.where(t < 2, core, 1 - core) * NH + i)
            return 0

        lax.fori_loop(0, 4, step, 0)
        return 0

    lax.fori_loop(0, NCH - NH, window2, 0)
    ostore(0, 0, 0).wait()
    ostore(0, 0, 1).wait()

    def drain(ch, _):
        y(ch).wait_send()
        s0(ch).wait_send()
        s1(ch).wait_send()

        @pl.when(diag)
        def _():
            p(ch).wait_send()

        @pl.when(diag == (ch < NH))
        def _():
            q_direct(ch).wait_send()
        return 0

    lax.fori_loop(0, NCH, drain, 0)


def last_back_kernel(a0, a1, b0, b1, z_ref, x_ref, gate_ref, gain_ref, proj_ref, prev_ref, o_ref, o_scr):
    back_body(pl.program_id(0), a0, a1, b0, b1, z_ref, x_ref, o_ref, gate_ref, gain_ref, proj_ref, o_scr)


def solution(mesh):
    tile_spec = P(('batch', 'row'), 'col', None)
    mask_spec = P(('batch', 'row'), 'col')
    repl_spec = P()
    any_spec = pl.BlockSpec(memory_space=pl.ANY)
    vmem_spec = pl.BlockSpec(memory_space=pltpu.VMEM)
    dma = pltpu.SemaphoreType.DMA
    out4 = jax.ShapeDtypeStruct((ROWS, 2, 2 * HALF, PAIR), BF16)

    def per_device(z_tile, mask_tile, ln_in_gain, proj_a, gate_a, proj_b, gate_b, gate_out, proj_out, ln_out_gain):
        mask = mask_tile.reshape(ROWS, 2, 2, HALF).transpose(0, 2, 1, 3).reshape(ROWS, COLS)
        gain_in = ln_in_gain.astype(F32).reshape(PAIR, 1)
        gain_out = ln_out_gain.astype(F32).reshape(HID, 1)
        z4 = z_tile.reshape(ROWS, 2, 2 * HALF, PAIR)

        def weights(proj, gate):
            both = jnp.stack([proj.T.reshape(HID // CH, CH, PAIR), gate.T.reshape(HID // CH, CH, PAIR)], axis=1)
            return both.reshape(2 * HID, PAIR) * 0.5

        w = jnp.stack([weights(proj_a, gate_a), weights(proj_b, gate_b)])
        gate_t, proj_t = gate_out.T, proj_out.T

        xb, g, xt, out = pl.pallas_call(
            main_kernel,
            out_shape=(
                jax.ShapeDtypeStruct((2, 3, ROWS, PAIR, COLS), BF16),
                jax.ShapeDtypeStruct((6, HID, ROWS, COLS), BF16),
                jax.ShapeDtypeStruct((ROWS, PAIR, COLS), BF16),
                out4,
            ),
            in_specs=[any_spec, any_spec] + [vmem_spec] * 6,
            out_specs=(any_spec,) * 4,
            scratch_shapes=[
                pltpu.VMEM((2, FB, COLS, PAIR), BF16),
                pltpu.VMEM((2, FB, PAIR, COLS), BF16),
                pltpu.VMEM((2, FB, PAIR, COLS), BF16),
                pltpu.VMEM((4, FB, PAIR, COLS), BF16),
                pltpu.VMEM((2, HID, FB, COLS), BF16),
                pltpu.VMEM((COLS // LANES, FB * PITCH, LANES), F32),
                pltpu.VMEM((HID * OPITCH, 2 * HALF), F32),
                dma((2,)), dma((2,)), dma((2,)), dma((4,)), dma((2,)),
            ] + [dma((NCH,))] * 10,
            compiler_params=pltpu.CompilerParams(vmem_limit_bytes=VMEM_LIMIT, collective_id=0, has_side_effects=True),
            name='exchange_project',
        )(z_tile, z4, mask, gain_in, w, gate_t, gain_out, proj_t)

        def whole(*shape):
            return pl.BlockSpec(shape, lambda s: (0,) * len(shape))

        specs, out_spec = back_specs(1)
        out = pl.pallas_call(
            last_back_kernel,
            grid=(N_C + N_I,),
            out_shape=out4,
            in_specs=specs + [whole(PAIR, PAIR), whole(HID, 1), whole(PAIR, HID), any_spec],
            out_specs=out_spec,
            scratch_shapes=[pltpu.VMEM((HID * OPITCH, 2 * HALF), F32)],
            input_output_aliases={9: 0},
            compiler_params=pltpu.CompilerParams(vmem_limit_bytes=VMEM_LIMIT),
            name='back',
        )(g, g, g, g, z4, xt, gate_t, gain_out, proj_t, out)
        return out.reshape(ROWS, COLS, PAIR)

    return jax.shard_map(per_device, mesh=mesh, in_specs=(tile_spec, mask_spec) + (repl_spec,) * 8, out_specs=tile_spec, check_vma=False)
```

```python
import jax
import jax.numpy as jnp
from jax import lax
from jax.experimental import pallas as pl
from jax.experimental.pallas import tpu as pltpu
from jax.sharding import PartitionSpec as P

LN_EPS = 1e-5
F32 = jnp.float32
BF16 = jnp.bfloat16
VMEM_LIMIT = 60 * 1024 * 1024
MESH = pl.DeviceIdType.MESH

ROWS, COLS, PAIR, HID = 128, 256, 128, 256
HALF = ROWS // 2
LANES = 128
FB = 16
NCH = ROWS // FB
NH = NCH // 2
CH = 128
PITCH = HID + 8
OPITCH = ROWS + 8
CB = 16
IB = 8
N_C, N_I = HID // CB, ROWS // IB


def normed_t(v, gain):
    mean = jnp.mean(v, axis=0, keepdims=True)
    cen = v - mean
    var = jnp.mean(cen * cen, axis=0, keepdims=True)
    return cen * lax.rsqrt(var + LN_EPS) * gain


def norm_chunk(z_ref, m_ref, first, gain, x_ref, xm_ref):
    for r in range(FB):
        z = z_ref[r].reshape(2, 2, HALF, PAIR)
        z = jnp.concatenate([z[0, 0], z[1, 0], z[0, 1], z[1, 1]], axis=0)
        x = normed_t(z.astype(F32).T, gain)
        x_ref[r] = x.astype(BF16)
        xm_ref[r] = (x * m_ref[pl.ds(first + r, 1), :].astype(F32)).astype(BF16)


def project_chunk(x_ref, w_ref, o_ref, scr):
    for r in range(FB):
        x = x_ref[r]
        for c in range(0, HID, CH):
            both = jnp.dot(w_ref[2 * c:2 * (c + CH), :], x, preferred_element_type=F32)
            proj = both[:CH]
            val = proj + jnp.tanh(both[CH:]) * proj
            for n in range(COLS // LANES):
                scr[n, pl.ds(r * PITCH + c, CH), :] = val[:, n * LANES:(n + 1) * LANES]

    def channel(c, _):
        for n in range(COLS // LANES):
            o_ref[c, :, n * LANES:(n + 1) * LANES] = scr[n, pl.ds(c, FB, stride=PITCH), :].astype(BF16)
        return 0

    lax.fori_loop(0, HID, channel, 0, unroll=16)


def column(row_ref):
    return row_ref[...].astype(F32).reshape(1, -1).T


def out_weights(gate_ref, gain_ref, proj_ref, gate_t, gain, proj_t):
    gate_t[...] = gate_ref[...].astype(F32).T.astype(BF16)
    gain[...] = column(gain_ref)
    proj_t[...] = proj_ref[...].astype(F32).T.astype(BF16)


def back_body(step, a0, a1, b0, b1, z_ref, x_ref, o_ref, gate_ref, gain_ref, proj_ref, o_scr):
    @pl.when(step < N_C)
    def _():
        for c in range(CB):
            dims = (((1,), (1,)), ((), ()))
            acc = lax.dot_general(a0[0, c], b0[0, c], dims, preferred_element_type=F32)
            acc = acc + lax.dot_general(a1[0, c], b1[0, c], dims, preferred_element_type=F32)
            o_scr[pl.ds(pl.multiple_of((step * CB + c) * OPITCH, 8), ROWS), :] = acc

    @pl.when(step >= N_C)
    def _():
        first = (step - N_C) * IB
        gain = gain_ref[...]

        def one_row(i, _):
            tri = o_scr[pl.ds(first + i, HID, stride=OPITCH), :]
            y = normed_t(tri, gain).astype(BF16)
            u = jnp.dot(proj_ref[...], y, preferred_element_type=F32)
            g = jax.nn.sigmoid(jnp.dot(gate_ref[...], x_ref[i], preferred_element_type=F32))
            z = z_ref[i].reshape(2 * HALF, PAIR).astype(F32)
            o_ref[i, :, o_ref.shape[2] - HALF:] = (z + (g * u).T).astype(BF16).reshape(2, HALF, PAIR)
            return 0

        lax.fori_loop(0, IB, one_row, 0, unroll=4)


def back_specs(half):
    def chan(slot):
        return pl.BlockSpec((1, CB, ROWS, COLS), lambda s: (slot, jnp.minimum(s, N_C - 1), 0, 0))

    tile = pl.BlockSpec((IB, 2, HALF, PAIR), lambda s: (jnp.maximum(s - N_C, 0), 0, half, 0))
    first = pl.BlockSpec((IB, 2, HALF, PAIR), lambda s: (jnp.maximum(s - N_C, 0), 0, 0, 0))
    x_spec = pl.BlockSpec((IB, PAIR, 2 * HALF), lambda s: (jnp.maximum(s - N_C, 0), 0, half))
    return [chan(0), chan(1), chan(2 + 2 * half), chan(3 + 2 * half), tile, x_spec], first


def main_kernel(z_ref, z4_ref, mask_in, gain_in, proj_a, gate_a, proj_b, gate_b, gate_in, gout_in, proj_in,
                xb, g_ref, xt, out_ref,
                mask_ref, w_ref, gate_ref, gout_ref, proj_ref, zbuf, xubuf, xmbuf, xin, obuf, scr, o_scr,
                zsem, xusem, xmsem, xsem, osem,
                y_s, p_s, q_s, s0_s, s1_s, y_r, p_r, q_r, s0_r, s1_r):
    row, col = lax.axis_index('row'), lax.axis_index('col')
    chip, core = row // 2, row % 2
    ydev = {'col': 1 - col}
    xdev = {'row': (1 - chip) * 2 + core}
    sdev = {'row': chip * 2 + 1 - core}
    diag = chip == col
    off = chip != col
    mine = 1 - diag.astype(jnp.int32)

    def part(k, slot, ch):
        return xb.at[k, slot, pl.ds(ch * FB, FB)]

    def rdma(src, dst, send, recv, dev):
        return pltpu.make_async_remote_copy(src_ref=src, dst_ref=dst, send_sem=send, recv_sem=recv,
                                            device_id=dev, device_id_type=MESH)

    def y(ch):
        return rdma(part(0, 0, ch), part(1, 0, ch), y_s.at[ch], y_r.at[ch], ydev)

    def p(ch):
        return rdma(part(0, 0, ch), part(0, 1, ch), p_s.at[ch], p_r.at[ch], xdev)

    def q_relay(ch):
        return rdma(part(1, 0, ch), part(1, 1, ch), q_s.at[ch], q_r.at[ch], xdev)

    def q_hop(ch):
        return rdma(part(0, 0, ch), part(1, 1, ch), q_s.at[ch], q_r.at[ch], xdev)

    def q_hop2(ch):
        return rdma(part(1, 1, ch), part(1, 1, ch), q_s.at[ch], q_r.at[ch], ydev)

    def s0(ch):
        return rdma(part(0, mine, ch), part(0, 2, ch), s0_s.at[ch], s0_r.at[ch], sdev)

    def s1(ch):
        return rdma(part(1, mine, ch), part(1, 2, ch), s1_s.at[ch], s1_r.at[ch], sdev)

    barrier = pltpu.get_barrier_semaphore()
    for dev in (ydev, xdev, sdev):
        pl.semaphore_signal(barrier, inc=1, device_id=dev, device_id_type=MESH)

    def zload(ch):
        return pltpu.make_async_copy(z_ref.at[pl.ds(ch * FB, FB)], zbuf.at[ch % 2], zsem.at[ch % 2])

    def xustore(ch):
        return pltpu.make_async_copy(xubuf.at[ch % 2], xt.at[pl.ds(ch * FB, FB)], xusem.at[ch % 2])

    def xmstore(ch):
        return pltpu.make_async_copy(xmbuf.at[ch % 2], part(0, 0, ch), xmsem.at[ch % 2])

    def publish(ch):
        xmstore(ch).wait()
        y(ch).start()

        @pl.when(diag)
        def _():
            s0(ch).start()

        @pl.when(diag & (ch < NH))
        def _():
            p(ch).start()

        @pl.when(off & (ch >= NH))
        def _():
            q_hop(ch).start()

    zload(0).start()
    gain = column(gain_in)
    mask = mask_in[...]
    mask_ref[...] = jnp.concatenate([mask[:, n * HALF:(n + 1) * HALF] for n in (0, 2, 1, 3)], axis=1)
    pl.semaphore_wait(barrier, 3)

    def norm_step(ch, _):
        @pl.when(ch + 1 < NCH)
        def _():
            zload(ch + 1).start()

        @pl.when(ch >= 2)
        def _():
            xustore(ch - 2).wait()

        zload(ch).wait()
        norm_chunk(zbuf.at[ch % 2], mask_ref, ch * FB, gain, xubuf.at[ch % 2], xmbuf.at[ch % 2])
        xustore(ch).start()
        xmstore(ch).start()

        @pl.when(ch >= 1)
        def _():
            publish(ch - 1)
        return 0

    lax.fori_loop(0, NCH, norm_step, 0)
    publish(NCH - 1)
    xustore(NCH - 2).wait()
    xustore(NCH - 1).wait()

    for n, (proj, gate) in enumerate(((proj_a, gate_a), (proj_b, gate_b))):
        for half, ref in ((0, proj), (1, gate)):
            w_t = (ref[...].astype(F32).T * 0.5).astype(BF16)
            for c in range(HID // CH):
                w_ref[n, pl.ds((2 * c + half) * CH, CH), :] = w_t[c * CH:(c + 1) * CH]
    out_weights(gate_in, gout_in, proj_in, gate_ref, gout_ref, proj_ref)

    def xload(k, slot, ch, t):
        return pltpu.make_async_copy(part(k, slot, ch), xin.at[t], xsem.at[t])

    def ostore(dst, block, t):
        return pltpu.make_async_copy(obuf.at[t % 2], g_ref.at[dst, :, pl.ds(block * FB, FB), :], osem.at[t % 2])

    def project(first_use, t, weight, dst, block):
        @pl.when(jnp.logical_not(first_use))
        def _():
            ostore(0, 0, t).wait()
        project_chunk(xin.at[t], w_ref.at[weight], obuf.at[t % 2], scr)
        ostore(dst, block, t).start()

    def window1(i, _):
        k, ch = i // NH, i % NH
        y(i).wait_recv()

        @pl.when(diag)
        def _():
            s1(i).start()

        @pl.when(diag & (i < NH))
        def _():
            q_relay(i).start()

        @pl.when(diag & (i == NH - 1))
        def _():
            for c in range(NH, NCH):
                p(c).start()

        @pl.when(diag & (i >= NH))
        def _():
            q_hop(i).wait_recv()
            q_hop2(i).start()

        @pl.when(off & (i < NH))
        def _():
            p(ch).wait_recv()
            s0(ch).start()

        @pl.when(off & (i >= NH))
        def _():
            q_relay(ch).wait_recv()
            s1(ch).start()

        xload(0, 0, i, 0).start()
        xload(1, 0, i, 1).start()
        xload(k, mine, ch, 2).start()

        def step(t, _):
            @pl.when((t == 1) & (i < NH))
            def _():
                s0(ch).wait_recv()

            @pl.when((t == 1) & (i >= NH))
            def _():
                s1(ch).wait_recv()

            @pl.when(t == 1)
            def _():
                xload(k, 2, ch, 3).start()

            xload(0, 0, 0, t).wait()
            is_b = t // 2
            own_block = jnp.where(t == 2, core, 1 - core) * NH + ch
            project((i == 0) & (t < 2), t, is_b, jnp.where(is_b == 1, 2 + k, t), jnp.where(is_b == 1, own_block, i))
            return 0

        lax.fori_loop(0, 4, step, 0)
        return 0

    lax.fori_loop(0, NCH, window1, 0)
    ostore(0, 0, 0).wait()
    ostore(0, 0, 1).wait()

    specs, out_spec = back_specs(0)

    def pipe(a0, a1, b0, b1, zr, xr, o):
        back_body(pl.program_id(0), a0, a1, b0, b1, zr, xr, o, gate_ref, gout_ref, proj_ref, o_scr)

    pltpu.emit_pipeline(pipe, grid=(N_C + N_I,), in_specs=specs, out_specs=[out_spec])(
        g_ref, g_ref, g_ref, g_ref, z4_ref, xt, out_ref)

    def window2(i, _):
        ch = NH + i

        @pl.when(off)
        def _():
            p(ch).wait_recv()
            s0(ch).start()
            q_hop2(ch).wait_recv()
            s1(ch).start()

        xload(0, mine, ch, 0).start()
        xload(1, mine, ch, 1).start()

        def step(t, _):
            @pl.when(t == 1)
            def _():
                s0(ch).wait_recv()
                xload(0, 2, ch, 2).start()
                s1(ch).wait_recv()
                xload(1, 2, ch, 3).start()

            xload(0, 0, 0, t).wait()
            project((i == 0) & (t < 2), t, 1, 4 + t % 2, jnp.where(t < 2, core, 1 - core) * NH + i)
            return 0

        lax.fori_loop(0, 4, step, 0)
        return 0

    lax.fori_loop(0, NCH - NH, window2, 0)
    ostore(0, 0, 0).wait()
    ostore(0, 0, 1).wait()

    def drain(ch, _):
        y(ch).wait_send()
        s0(ch).wait_send()
        s1(ch).wait_send()

        @pl.when(diag)
        def _():
            p(ch).wait_send()

        @pl.when(diag | (ch >= NH))
        def _():
            q_hop(ch).wait_send()
        return 0

    lax.fori_loop(0, NCH, drain, 0)


def last_back_kernel(a0, a1, b0, b1, z_ref, x_ref, gate_ref, gain_ref, proj_ref, first_ref, o_ref, gate_t, gain, proj_t, o_scr):
    step = pl.program_id(0)

    @pl.when(step == 0)
    def _():
        out_weights(gate_ref, gain_ref, proj_ref, gate_t, gain, proj_t)

    @pl.when(step >= N_C)
    def _():
        o_ref[:, :, :HALF] = first_ref[...]
    back_body(step, a0, a1, b0, b1, z_ref, x_ref, o_ref, gate_t, gain, proj_t, o_scr)


def solution(mesh):
    tile_spec = P(('batch', 'row'), 'col', None)
    mask_spec = P(('batch', 'row'), 'col')
    repl_spec = P()
    any_spec = pl.BlockSpec(memory_space=pl.ANY)
    vmem_spec = pl.BlockSpec(memory_space=pltpu.VMEM)
    dma = pltpu.SemaphoreType.DMA

    def per_device(z_tile, mask_tile, ln_in_gain, proj_a, gate_a, proj_b, gate_b, gate_out, proj_out, ln_out_gain):
        gain_in, gain_out = ln_in_gain.reshape(1, PAIR), ln_out_gain.reshape(1, HID)
        z4 = z_tile.reshape(ROWS, 2, 2 * HALF, PAIR)
        out_w = [pltpu.VMEM((PAIR, PAIR), BF16), pltpu.VMEM((HID, 1), F32), pltpu.VMEM((PAIR, HID), BF16)]

        _, g, xt, first = pl.pallas_call(
            main_kernel,
            out_shape=(
                jax.ShapeDtypeStruct((2, 3, ROWS, PAIR, COLS), BF16),
                jax.ShapeDtypeStruct((6, HID, ROWS, COLS), BF16),
                jax.ShapeDtypeStruct((ROWS, PAIR, COLS), BF16),
                jax.ShapeDtypeStruct((ROWS, 2, HALF, PAIR), BF16),
            ),
            in_specs=[any_spec, any_spec] + [vmem_spec] * 9,
            out_specs=(any_spec,) * 4,
            scratch_shapes=[
                pltpu.VMEM((ROWS, COLS), jnp.int32),
                pltpu.VMEM((2, 2 * HID, PAIR), BF16),
                *out_w,
                pltpu.VMEM((2, FB, COLS, PAIR), BF16),
                pltpu.VMEM((2, FB, PAIR, COLS), BF16),
                pltpu.VMEM((2, FB, PAIR, COLS), BF16),
                pltpu.VMEM((4, FB, PAIR, COLS), BF16),
                pltpu.VMEM((2, HID, FB, COLS), BF16),
                pltpu.VMEM((COLS // LANES, FB * PITCH, LANES), F32),
                pltpu.VMEM((HID * OPITCH, 2 * HALF), F32),
                dma((2,)), dma((2,)), dma((2,)), dma((4,)), dma((2,)),
            ] + [dma((NCH,))] * 10,
            compiler_params=pltpu.CompilerParams(vmem_limit_bytes=VMEM_LIMIT, collective_id=0, has_side_effects=True),
            name='exchange_project',
        )(z_tile, z4, mask_tile, gain_in, proj_a, gate_a, proj_b, gate_b, gate_out, gain_out, proj_out)

        def whole(*shape):
            return pl.BlockSpec(shape, lambda s: (0,) * len(shape))

        specs, first_spec = back_specs(1)
        out = pl.pallas_call(
            last_back_kernel,
            grid=(N_C + N_I,),
            out_shape=jax.ShapeDtypeStruct((ROWS, 2, 2 * HALF, PAIR), BF16),
            in_specs=specs + [whole(PAIR, PAIR), whole(1, HID), whole(HID, PAIR), first_spec],
            out_specs=pl.BlockSpec((IB, 2, 2 * HALF, PAIR), lambda s: (jnp.maximum(s - N_C, 0), 0, 0, 0)),
            scratch_shapes=[*out_w, pltpu.VMEM((HID * OPITCH, 2 * HALF), F32)],
            compiler_params=pltpu.CompilerParams(vmem_limit_bytes=VMEM_LIMIT),
            name='back',
        )(g, g, g, g, z4, xt, gate_out, gain_out, proj_out, first)
        return out.reshape(ROWS, COLS, PAIR)

    return jax.shard_map(per_device, mesh=mesh, in_specs=(tile_spec, mask_spec) + (repl_spec,) * 8, out_specs=tile_spec, check_vma=False)
```

```python
import jax
import jax.numpy as jnp
from jax import lax
from jax.experimental import pallas as pl
from jax.experimental.pallas import tpu as pltpu
from jax.sharding import PartitionSpec as P

LN_EPS = 1e-5
F32 = jnp.float32
BF16 = jnp.bfloat16
VMEM_LIMIT = 60 * 1024 * 1024
MESH = pl.DeviceIdType.MESH

ROWS, COLS, PAIR, HID = 128, 256, 128, 256
HALF = ROWS // 2
LANES = 128
FB = 16
NCH = ROWS // FB
NH = NCH // 2
CH = 128
PITCH = HID + 4
OPITCH = ROWS + 8
CB = 32
IB = 16
N_C, N_I = HID // CB, ROWS // IB


def normed_t(v, gain):
    mean = jnp.mean(v, axis=0, keepdims=True)
    cen = v - mean
    var = jnp.mean(cen * cen, axis=0, keepdims=True)
    return cen * lax.rsqrt(var + LN_EPS) * gain


def norm_chunk(z_ref, m_ref, first, gain, x_ref, xm_ref):
    for r in range(FB):
        z = z_ref[r].reshape(2, 2, HALF, PAIR)
        z = jnp.concatenate([z[0, 0], z[1, 0], z[0, 1], z[1, 1]], axis=0)
        x = normed_t(z.astype(F32).T, gain)
        x_ref[r] = x.astype(BF16)
        xm_ref[r] = (x * m_ref[pl.ds(first + r, 1), :].astype(F32)).astype(BF16)


def project_chunk(x_ref, w_ref, o_ref, scr):
    for r in range(FB):
        x = x_ref[r]
        for c in range(0, HID, CH):
            both = jnp.dot(w_ref[2 * c:2 * (c + CH), :], x, preferred_element_type=F32)
            proj = both[:CH]
            val = proj + jnp.tanh(both[CH:]) * proj
            for n in range(COLS // LANES):
                scr[n, pl.ds(r * PITCH + c, CH), :] = val[:, n * LANES:(n + 1) * LANES]

    def channel(c, _):
        for n in range(COLS // LANES):
            o_ref[c, :, n * LANES:(n + 1) * LANES] = scr[n, pl.ds(c, FB, stride=PITCH), :].astype(BF16)
        return 0

    lax.fori_loop(0, HID, channel, 0, unroll=16)


def column(row_ref):
    return row_ref[...].astype(F32).reshape(1, -1).T


def out_weights(gate_ref, gain_ref, proj_ref, gate_t, gain, proj_t):
    gate_t[...] = gate_ref[...].astype(F32).T.astype(BF16)
    gain[...] = column(gain_ref)
    proj_t[...] = proj_ref[...].astype(F32).T.astype(BF16)


def back_body(step, a0, a1, b0, b1, z_ref, x_ref, o_ref, gate_ref, gain_ref, proj_ref, o_scr):
    @pl.when(step < N_C)
    def _():
        for c in range(CB):
            dims = (((1,), (1,)), ((), ()))
            acc = lax.dot_general(a0[0, c], b0[0, c], dims, preferred_element_type=F32)
            acc = acc + lax.dot_general(a1[0, c], b1[0, c], dims, preferred_element_type=F32)
            o_scr[pl.ds(pl.multiple_of((step * CB + c) * OPITCH, 8), ROWS), :] = acc

    @pl.when(step >= N_C)
    def _():
        first = (step - N_C) * IB
        gain = gain_ref[...]

        def one_row(i, _):
            tri = o_scr[pl.ds(first + i, HID, stride=OPITCH), :]
            y = normed_t(tri, gain).astype(BF16)
            u = jnp.dot(proj_ref[...], y, preferred_element_type=F32)
            g = jax.nn.sigmoid(jnp.dot(gate_ref[...], x_ref[i], preferred_element_type=F32))
            z = z_ref[i].reshape(2 * HALF, PAIR).astype(F32)
            o_ref[i, :, o_ref.shape[2] - HALF:] = (z + (g * u).T).astype(BF16).reshape(2, HALF, PAIR)
            return 0

        lax.fori_loop(0, IB, one_row, 0, unroll=16)


def back_specs(half):
    def chan(slot):
        return pl.BlockSpec((1, CB, ROWS, COLS), lambda s: (slot, jnp.minimum(s, N_C - 1), 0, 0))

    tile = pl.BlockSpec((IB, 2, HALF, PAIR), lambda s: (jnp.maximum(s - N_C, 0), 0, half, 0))
    first = pl.BlockSpec((IB, 2, HALF, PAIR), lambda s: (jnp.maximum(s - N_C, 0), 0, 0, 0))
    x_spec = pl.BlockSpec((IB, PAIR, 2 * HALF), lambda s: (jnp.maximum(s - N_C, 0), 0, half))
    return [chan(0), chan(1), chan(2 + 2 * half), chan(3 + 2 * half), tile, x_spec], first


def main_kernel(z_ref, z4_ref, mask_in, gain_in, proj_a, gate_a, proj_b, gate_b, gate_in, gout_in, proj_in,
                xb, g_ref, xt, out_ref,
                mask_ref, w_ref, gate_ref, gout_ref, proj_ref, zbuf, xubuf, xmbuf, xin, obuf, scr, o_scr,
                zsem, xusem, xmsem, xsem, osem,
                y_s, p_s, q_s, s0_s, s1_s, y_r, p_r, q_r, s0_r, s1_r):
    row, col = lax.axis_index('row'), lax.axis_index('col')
    chip, core = row // 2, row % 2
    ydev = {'col': 1 - col}
    xdev = {'row': (1 - chip) * 2 + core}
    sdev = {'row': chip * 2 + 1 - core}
    diag = chip == col
    off = chip != col
    mine = 1 - diag.astype(jnp.int32)

    def part(k, slot, ch):
        return xb.at[k, slot, pl.ds(ch * FB, FB)]

    def rdma(src, dst, send, recv, dev):
        return pltpu.make_async_remote_copy(src_ref=src, dst_ref=dst, send_sem=send, recv_sem=recv,
                                            device_id=dev, device_id_type=MESH)

    def y(ch):
        return rdma(part(0, 0, ch), part(1, 0, ch), y_s.at[ch], y_r.at[ch], ydev)

    def p(ch):
        return rdma(part(0, 0, ch), part(0, 1, ch), p_s.at[ch], p_r.at[ch], xdev)

    def q_relay(ch):
        return rdma(part(1, 0, ch), part(1, 1, ch), q_s.at[ch], q_r.at[ch], xdev)

    def q_hop(ch):
        return rdma(part(0, 0, ch), part(1, 1, ch), q_s.at[ch], q_r.at[ch], xdev)

    def q_hop2(ch):
        return rdma(part(1, 1, ch), part(1, 1, ch), q_s.at[ch], q_r.at[ch], ydev)

    def s0(ch):
        return rdma(part(0, mine, ch), part(0, 2, ch), s0_s.at[ch], s0_r.at[ch], sdev)

    def s1(ch):
        return rdma(part(1, mine, ch), part(1, 2, ch), s1_s.at[ch], s1_r.at[ch], sdev)

    barrier = pltpu.get_barrier_semaphore()
    for dev in (ydev, xdev, sdev):
        pl.semaphore_signal(barrier, inc=1, device_id=dev, device_id_type=MESH)

    def zload(ch):
        return pltpu.make_async_copy(z_ref.at[pl.ds(ch * FB, FB)], zbuf.at[ch % 2], zsem.at[ch % 2])

    def xustore(ch):
        return pltpu.make_async_copy(xubuf.at[ch % 2], xt.at[pl.ds(ch * FB, FB)], xusem.at[ch % 2])

    def xmstore(ch):
        return pltpu.make_async_copy(xmbuf.at[ch % 2], part(0, 0, ch), xmsem.at[ch % 2])

    def publish(ch):
        xmstore(ch).wait()
        y(ch).start()

        @pl.when(diag)
        def _():
            s0(ch).start()

        @pl.when(diag & (ch < NH))
        def _():
            p(ch).start()

        @pl.when(off & (ch >= NH))
        def _():
            q_hop(ch).start()

    zload(0).start()
    gain = column(gain_in)
    mask = mask_in[...]
    mask_ref[...] = jnp.concatenate([mask[:, n * HALF:(n + 1) * HALF] for n in (0, 2, 1, 3)], axis=1)
    pl.semaphore_wait(barrier, 3)

    def norm_step(ch, _):
        @pl.when(ch + 1 < NCH)
        def _():
            zload(ch + 1).start()

        @pl.when(ch >= 2)
        def _():
            xustore(ch - 2).wait()

        zload(ch).wait()
        norm_chunk(zbuf.at[ch % 2], mask_ref, ch * FB, gain, xubuf.at[ch % 2], xmbuf.at[ch % 2])
        xustore(ch).start()
        xmstore(ch).start()

        @pl.when(ch >= 1)
        def _():
            publish(ch - 1)
        return 0

    lax.fori_loop(0, NCH, norm_step, 0)
    publish(NCH - 1)
    xustore(NCH - 2).wait()
    xustore(NCH - 1).wait()

    for n, (proj, gate) in enumerate(((proj_a, gate_a), (proj_b, gate_b))):
        for half, ref in ((0, proj), (1, gate)):
            w_t = (ref[...].astype(F32).T * 0.5).astype(BF16)
            for c in range(HID // CH):
                w_ref[n, pl.ds((2 * c + half) * CH, CH), :] = w_t[c * CH:(c + 1) * CH]
    out_weights(gate_in, gout_in, proj_in, gate_ref, gout_ref, proj_ref)

    def xload(k, slot, ch, t):
        return pltpu.make_async_copy(part(k, slot, ch), xin.at[t], xsem.at[t])

    def ostore(dst, block, t):
        return pltpu.make_async_copy(obuf.at[t % 2], g_ref.at[dst, :, pl.ds(block * FB, FB), :], osem.at[t % 2])

    def project(first_use, t, weight, dst, block):
        @pl.when(jnp.logical_not(first_use))
        def _():
            ostore(0, 0, t).wait()
        project_chunk(xin.at[t], w_ref.at[weight], obuf.at[t % 2], scr)
        ostore(dst, block, t).start()

    def window1(i, _):
        k, ch = i // NH, i % NH
        y(i).wait_recv()

        @pl.when(diag)
        def _():
            s1(i).start()

        @pl.when(diag & (i < NH))
        def _():
            q_relay(i).start()

        @pl.when(diag & (i == NH - 1))
        def _():
            for c in range(NH, NCH):
                p(c).start()

        @pl.when(diag & (i >= NH))
        def _():
            q_hop(i).wait_recv()
            q_hop2(i).start()

        @pl.when(off & (i < NH))
        def _():
            p(ch).wait_recv()
            s0(ch).start()

        @pl.when(off & (i >= NH))
        def _():
            q_relay(ch).wait_recv()
            s1(ch).start()

        xload(0, 0, i, 0).start()
        xload(1, 0, i, 1).start()
        xload(k, mine, ch, 2).start()

        def step(t, _):
            @pl.when((t == 1) & (i < NH))
            def _():
                s0(ch).wait_recv()

            @pl.when((t == 1) & (i >= NH))
            def _():
                s1(ch).wait_recv()

            @pl.when(t == 1)
            def _():
                xload(k, 2, ch, 3).start()

            xload(0, 0, 0, t).wait()
            is_b = t // 2
            own_block = jnp.where(t == 2, core, 1 - core) * NH + ch
            project((i == 0) & (t < 2), t, is_b, jnp.where(is_b == 1, 2 + k, t), jnp.where(is_b == 1, own_block, i))
            return 0

        lax.fori_loop(0, 4, step, 0)
        return 0

    lax.fori_loop(0, NCH, window1, 0)
    ostore(0, 0, 0).wait()
    ostore(0, 0, 1).wait()

    specs, out_spec = back_specs(0)

    def pipe(a0, a1, b0, b1, zr, xr, o):
        back_body(pl.program_id(0), a0, a1, b0, b1, zr, xr, o, gate_ref, gout_ref, proj_ref, o_scr)

    pltpu.emit_pipeline(pipe, grid=(N_C + N_I,), in_specs=specs, out_specs=[out_spec])(
        g_ref, g_ref, g_ref, g_ref, z4_ref, xt, out_ref)

    def window2(i, _):
        ch = NH + i

        @pl.when(off)
        def _():
            p(ch).wait_recv()
            s0(ch).start()
            q_hop2(ch).wait_recv()
            s1(ch).start()

        xload(0, mine, ch, 0).start()
        xload(1, mine, ch, 1).start()

        def step(t, _):
            @pl.when(t == 1)
            def _():
                s0(ch).wait_recv()
                xload(0, 2, ch, 2).start()
                s1(ch).wait_recv()
                xload(1, 2, ch, 3).start()

            xload(0, 0, 0, t).wait()
            project((i == 0) & (t < 2), t, 1, 4 + t % 2, jnp.where(t < 2, core, 1 - core) * NH + i)
            return 0

        lax.fori_loop(0, 4, step, 0)
        return 0

    lax.fori_loop(0, NCH - NH, window2, 0)
    ostore(0, 0, 0).wait()
    ostore(0, 0, 1).wait()

    def drain(ch, _):
        y(ch).wait_send()
        s0(ch).wait_send()
        s1(ch).wait_send()

        @pl.when(diag)
        def _():
            p(ch).wait_send()

        @pl.when(diag | (ch >= NH))
        def _():
            q_hop(ch).wait_send()
        return 0

    lax.fori_loop(0, NCH, drain, 0)


def last_back_kernel(a0, a1, b0, b1, z_ref, x_ref, gate_ref, gain_ref, proj_ref, first_ref, o_ref, gate_t, gain, proj_t, o_scr):
    step = pl.program_id(0)

    @pl.when(step == 0)
    def _():
        out_weights(gate_ref, gain_ref, proj_ref, gate_t, gain, proj_t)

    @pl.when(step >= N_C)
    def _():
        o_ref[:, :, :HALF] = first_ref[...]
    back_body(step, a0, a1, b0, b1, z_ref, x_ref, o_ref, gate_t, gain, proj_t, o_scr)


def solution(mesh):
    tile_spec = P(('batch', 'row'), 'col', None)
    mask_spec = P(('batch', 'row'), 'col')
    repl_spec = P()
    any_spec = pl.BlockSpec(memory_space=pl.ANY)
    vmem_spec = pl.BlockSpec(memory_space=pltpu.VMEM)
    dma = pltpu.SemaphoreType.DMA

    def per_device(z_tile, mask_tile, ln_in_gain, proj_a, gate_a, proj_b, gate_b, gate_out, proj_out, ln_out_gain):
        gain_in, gain_out = ln_in_gain.reshape(1, PAIR), ln_out_gain.reshape(1, HID)
        z4 = z_tile.reshape(ROWS, 2, 2 * HALF, PAIR)
        out_w = [pltpu.VMEM((PAIR, PAIR), BF16), pltpu.VMEM((HID, 1), F32), pltpu.VMEM((PAIR, HID), BF16)]

        _, g, xt, first = pl.pallas_call(
            main_kernel,
            out_shape=(
                jax.ShapeDtypeStruct((2, 3, ROWS, PAIR, COLS), BF16),
                jax.ShapeDtypeStruct((6, HID, ROWS, COLS), BF16),
                jax.ShapeDtypeStruct((ROWS, PAIR, COLS), BF16),
                jax.ShapeDtypeStruct((ROWS, 2, HALF, PAIR), BF16),
            ),
            in_specs=[any_spec, any_spec] + [vmem_spec] * 9,
            out_specs=(any_spec,) * 4,
            scratch_shapes=[
                pltpu.VMEM((ROWS, COLS), jnp.int32),
                pltpu.VMEM((2, 2 * HID, PAIR), BF16),
                *out_w,
                pltpu.VMEM((2, FB, COLS, PAIR), BF16),
                pltpu.VMEM((2, FB, PAIR, COLS), BF16),
                pltpu.VMEM((2, FB, PAIR, COLS), BF16),
                pltpu.VMEM((4, FB, PAIR, COLS), BF16),
                pltpu.VMEM((2, HID, FB, COLS), BF16),
                pltpu.VMEM((COLS // LANES, FB * PITCH, LANES), F32),
                pltpu.VMEM((HID * OPITCH, 2 * HALF), F32),
                dma((2,)), dma((2,)), dma((2,)), dma((4,)), dma((2,)),
            ] + [dma((NCH,))] * 10,
            compiler_params=pltpu.CompilerParams(vmem_limit_bytes=VMEM_LIMIT, collective_id=0, has_side_effects=True),
            name='exchange_project',
        )(z_tile, z4, mask_tile, gain_in, proj_a, gate_a, proj_b, gate_b, gate_out, gain_out, proj_out)

        def whole(*shape):
            return pl.BlockSpec(shape, lambda s: (0,) * len(shape))

        specs, first_spec = back_specs(1)
        out = pl.pallas_call(
            last_back_kernel,
            grid=(N_C + N_I,),
            out_shape=jax.ShapeDtypeStruct((ROWS, 2, 2 * HALF, PAIR), BF16),
            in_specs=specs + [whole(PAIR, PAIR), whole(1, HID), whole(HID, PAIR), first_spec],
            out_specs=pl.BlockSpec((IB, 2, 2 * HALF, PAIR), lambda s: (jnp.maximum(s - N_C, 0), 0, 0, 0)),
            scratch_shapes=[*out_w, pltpu.VMEM((HID * OPITCH, 2 * HALF), F32)],
            compiler_params=pltpu.CompilerParams(vmem_limit_bytes=VMEM_LIMIT),
            name='back',
        )(g, g, g, g, z4, xt, gate_out, gain_out, proj_out, first)
        return out.reshape(ROWS, COLS, PAIR)

    return jax.shard_map(per_device, mesh=mesh, in_specs=(tile_spec, mask_spec) + (repl_spec,) * 8, out_specs=tile_spec, check_vma=False)
```

```python
import jax
import jax.numpy as jnp
from jax import lax
from jax.experimental import pallas as pl
from jax.experimental.pallas import tpu as pltpu
from jax.sharding import PartitionSpec as P

LN_EPS = 1e-5
F32 = jnp.float32
BF16 = jnp.bfloat16
VMEM_LIMIT = 60 * 1024 * 1024
MESH = pl.DeviceIdType.MESH

ROWS, COLS, PAIR, HID = 128, 256, 128, 256
HALF = ROWS // 2
LANES = 128
FB = 16
NCH = ROWS // FB
NH = NCH // 2
CH = 128
PITCH = HID + 4
OPITCH = ROWS + 4
CB = 32
IB = 16
N_C, N_I = HID // CB, ROWS // IB


def normed_t(v, gain):
    mean = jnp.mean(v, axis=0, keepdims=True)
    cen = v - mean
    var = jnp.mean(cen * cen, axis=0, keepdims=True)
    return cen * lax.rsqrt(var + LN_EPS) * gain


def norm_chunk(z_ref, m_ref, first, gain, x_ref, xm_ref):
    for r in range(FB):
        z = z_ref[r].reshape(2, 2, HALF, PAIR)
        z = jnp.concatenate([z[0, 0], z[1, 0], z[0, 1], z[1, 1]], axis=0)
        x = normed_t(z.astype(F32).T, gain)
        x_ref[r] = x.astype(BF16)
        xm_ref[r] = (x * m_ref[pl.ds(first + r, 1), :].astype(F32)).astype(BF16)


def project_chunk(x_ref, w_ref, o_ref, scr):
    for r in range(FB):
        x = x_ref[r]
        for c in range(0, HID, CH):
            both = jnp.dot(w_ref[2 * c:2 * (c + CH), :], x, preferred_element_type=F32)
            proj = both[:CH]
            val = proj + jnp.tanh(both[CH:]) * proj
            for n in range(COLS // LANES):
                scr[n, pl.ds(r * PITCH + c, CH), :] = val[:, n * LANES:(n + 1) * LANES]

    def channel(c, _):
        for n in range(COLS // LANES):
            o_ref[c, :, n * LANES:(n + 1) * LANES] = scr[n, pl.ds(c, FB, stride=PITCH), :].astype(BF16)
        return 0

    lax.fori_loop(0, HID, channel, 0, unroll=16)


def column(row_ref):
    cols = row_ref[...].astype(F32).T
    return jnp.concatenate([cols[:, n:n + 1] for n in range(cols.shape[1])], axis=0)


def out_weights(gate_ref, gain_ref, proj_ref, gate_t, gain, proj_t):
    gate_t[...] = (gate_ref[...].astype(F32).T * 0.5).astype(BF16)
    gain[...] = column(gain_ref)
    proj_t[...] = (proj_ref[...].astype(F32).T * 0.5).astype(BF16)


def back_body(step, a0, a1, b0, b1, z_ref, x_ref, o_ref, gate_ref, gain_ref, proj_ref, o_scr):
    @pl.when(step < N_C)
    def _():
        for c in range(CB):
            dims = (((1,), (1,)), ((), ()))
            acc = lax.dot_general(a0[0, c], b0[0, c], dims, preferred_element_type=F32)
            acc = acc + lax.dot_general(a1[0, c], b1[0, c], dims, preferred_element_type=F32)
            o_scr[pl.ds(pl.multiple_of((step * CB + c) * OPITCH, 4), ROWS), :] = acc

    @pl.when(step >= N_C)
    def _():
        first = (step - N_C) * IB
        gain = gain_ref[...]

        def one_row(i, _):
            tri = o_scr[pl.ds(first + i, HID, stride=OPITCH), :]
            y = normed_t(tri, gain).astype(BF16)
            u = jnp.dot(proj_ref[...], y, preferred_element_type=F32)
            t = jnp.tanh(jnp.dot(gate_ref[...], x_ref[i], preferred_element_type=F32))
            z = z_ref[i].reshape(2 * HALF, PAIR).astype(F32)
            o_ref[i, :, o_ref.shape[2] - HALF:] = (z + (u + t * u).T).astype(BF16).reshape(2, HALF, PAIR)
            return 0

        lax.fori_loop(0, IB, one_row, 0, unroll=16)


def back_specs(half):
    def chan(slot):
        return pl.BlockSpec((1, CB, ROWS, COLS), lambda s: (slot, jnp.minimum(s, N_C - 1), 0, 0))

    tile = pl.BlockSpec((IB, 2, HALF, PAIR), lambda s: (jnp.maximum(s - N_C, 0), 0, half, 0))
    first = pl.BlockSpec((IB, 2, HALF, PAIR), lambda s: (jnp.maximum(s - N_C, 0), 0, 0, 0))
    x_spec = pl.BlockSpec((IB, PAIR, 2 * HALF), lambda s: (jnp.maximum(s - N_C, 0), 0, half))
    return [chan(0), chan(1), chan(2 + 2 * half), chan(3 + 2 * half), tile, x_spec], first


def main_kernel(z_ref, z4_ref, mask_in, gain_in, proj_a, gate_a, proj_b, gate_b, gate_in, gout_in, proj_in,
                xb, g_ref, xt, out_ref,
                mask_ref, w_ref, gate_ref, gout_ref, proj_ref, zbuf, xubuf, xmbuf, xin, obuf, scr, o_scr,
                zsem, xusem, xmsem, xsem, osem,
                y_s, p_s, q_s, s0_s, s1_s, y_r, p_r, q_r, s0_r, s1_r):
    row, col = lax.axis_index('row'), lax.axis_index('col')
    chip, core = row // 2, row % 2
    ydev = {'col': 1 - col}
    xdev = {'row': (1 - chip) * 2 + core}
    sdev = {'row': chip * 2 + 1 - core}
    diag = chip == col
    off = chip != col
    mine = 1 - diag.astype(jnp.int32)

    def part(k, slot, ch):
        return xb.at[k, slot, pl.ds(ch * FB, FB)]

    def rdma(src, dst, send, recv, dev):
        return pltpu.make_async_remote_copy(src_ref=src, dst_ref=dst, send_sem=send, recv_sem=recv,
                                            device_id=dev, device_id_type=MESH)

    def y(ch):
        return rdma(part(0, 0, ch), part(1, 0, ch), y_s.at[ch], y_r.at[ch], ydev)

    def p(ch):
        return rdma(part(0, 0, ch), part(0, 1, ch), p_s.at[ch], p_r.at[ch], xdev)

    def q_relay(ch):
        return rdma(part(1, 0, ch), part(1, 1, ch), q_s.at[ch], q_r.at[ch], xdev)

    def q_hop(ch):
        return rdma(part(0, 0, ch), part(1, 1, ch), q_s.at[ch], q_r.at[ch], xdev)

    def q_hop2(ch):
        return rdma(part(1, 1, ch), part(1, 1, ch), q_s.at[ch], q_r.at[ch], ydev)

    def s0(ch):
        return rdma(part(0, mine, ch), part(0, 2, ch), s0_s.at[ch], s0_r.at[ch], sdev)

    def s1(ch):
        return rdma(part(1, mine, ch), part(1, 2, ch), s1_s.at[ch], s1_r.at[ch], sdev)

    barrier = pltpu.get_barrier_semaphore()
    for dev in (ydev, xdev, sdev):
        pl.semaphore_signal(barrier, inc=1, device_id=dev, device_id_type=MESH)

    def zload(ch):
        return pltpu.make_async_copy(z_ref.at[pl.ds(ch * FB, FB)], zbuf.at[ch % 2], zsem.at[ch % 2])

    def xustore(ch):
        return pltpu.make_async_copy(xubuf.at[ch % 2], xt.at[pl.ds(ch * FB, FB)], xusem.at[ch % 2])

    def xmstore(ch):
        return pltpu.make_async_copy(xmbuf.at[ch % 2], part(0, 0, ch), xmsem.at[ch % 2])

    def publish(ch):
        xmstore(ch).wait()
        y(ch).start()

        @pl.when(diag)
        def _():
            s0(ch).start()

        @pl.when(diag & (ch < NH))
        def _():
            p(ch).start()

        @pl.when(off & (ch >= NH))
        def _():
            q_hop(ch).start()

    zload(0).start()
    gain = column(gain_in)
    mask = mask_in[...]
    mask_ref[...] = jnp.concatenate([mask[:, n * HALF:(n + 1) * HALF] for n in (0, 2, 1, 3)], axis=1)
    pl.semaphore_wait(barrier, 3)

    def norm_step(ch, _):
        @pl.when(ch + 1 < NCH)
        def _():
            zload(ch + 1).start()

        @pl.when(ch >= 2)
        def _():
            xustore(ch - 2).wait()

        zload(ch).wait()
        norm_chunk(zbuf.at[ch % 2], mask_ref, ch * FB, gain, xubuf.at[ch % 2], xmbuf.at[ch % 2])
        xustore(ch).start()
        xmstore(ch).start()

        @pl.when(ch == 0)
        def _():
            publish(0)

        @pl.when(ch >= 2)
        def _():
            publish(ch - 1)
        return 0

    lax.fori_loop(0, NCH, norm_step, 0)
    publish(NCH - 1)
    xustore(NCH - 2).wait()
    xustore(NCH - 1).wait()

    for n, (proj, gate) in enumerate(((proj_a, gate_a), (proj_b, gate_b))):
        for half, ref in ((0, proj), (1, gate)):
            w_t = (ref[...].astype(F32).T * 0.5).astype(BF16)
            for c in range(HID // CH):
                w_ref[n, pl.ds((2 * c + half) * CH, CH), :] = w_t[c * CH:(c + 1) * CH]
    out_weights(gate_in, gout_in, proj_in, gate_ref, gout_ref, proj_ref)

    def xload(k, slot, ch, t):
        return pltpu.make_async_copy(part(k, slot, ch), xin.at[t], xsem.at[t])

    def ostore(dst, block, t):
        return pltpu.make_async_copy(obuf.at[t % 2], g_ref.at[dst, :, pl.ds(block * FB, FB), :], osem.at[t % 2])

    def project(first_use, t, weight, dst, block):
        @pl.when(jnp.logical_not(first_use))
        def _():
            ostore(0, 0, t).wait()
        project_chunk(xin.at[t], w_ref.at[weight], obuf.at[t % 2], scr)
        ostore(dst, block, t).start()

    def window1(i, _):
        k, ch = i // NH, i % NH
        y(i).wait_recv()

        @pl.when(diag)
        def _():
            s1(i).start()

        @pl.when(diag & (i < NH))
        def _():
            q_relay(i).start()

        @pl.when(diag & (i == NH - 1))
        def _():
            for c in range(NH, NCH):
                p(c).start()

        @pl.when(diag & (i >= NH))
        def _():
            q_hop(i).wait_recv()
            q_hop2(i).start()

        @pl.when(off & (i < NH))
        def _():
            p(ch).wait_recv()
            s0(ch).start()

        @pl.when(off & (i >= NH))
        def _():
            q_relay(ch).wait_recv()
            s1(ch).start()

        xload(0, 0, i, 0).start()
        xload(1, 0, i, 1).start()
        xload(k, mine, ch, 2).start()

        def step(t, _):
            @pl.when((t == 1) & (i < NH))
            def _():
                s0(ch).wait_recv()

            @pl.when((t == 1) & (i >= NH))
            def _():
                s1(ch).wait_recv()

            @pl.when(t == 1)
            def _():
                xload(k, 2, ch, 3).start()

            xload(0, 0, 0, t).wait()
            is_b = t // 2
            own_block = jnp.where(t == 2, core, 1 - core) * NH + ch
            project((i == 0) & (t < 2), t, is_b, jnp.where(is_b == 1, 2 + k, t), jnp.where(is_b == 1, own_block, i))
            return 0

        lax.fori_loop(0, 4, step, 0)
        return 0

    lax.fori_loop(0, NCH, window1, 0)
    ostore(0, 0, 0).wait()
    ostore(0, 0, 1).wait()

    specs, out_spec = back_specs(0)

    def pipe(a0, a1, b0, b1, zr, xr, o):
        back_body(pl.program_id(0), a0, a1, b0, b1, zr, xr, o, gate_ref, gout_ref, proj_ref, o_scr)

    pltpu.emit_pipeline(pipe, grid=(N_C + N_I,), in_specs=specs, out_specs=[out_spec])(
        g_ref, g_ref, g_ref, g_ref, z4_ref, xt, out_ref)

    def window2(i, _):
        ch = NH + i

        @pl.when(off)
        def _():
            p(ch).wait_recv()
            s0(ch).start()
            q_hop2(ch).wait_recv()
            s1(ch).start()

        xload(0, mine, ch, 0).start()
        xload(1, mine, ch, 1).start()

        def step(t, _):
            @pl.when(t == 1)
            def _():
                s0(ch).wait_recv()
                xload(0, 2, ch, 2).start()
                s1(ch).wait_recv()
                xload(1, 2, ch, 3).start()

            xload(0, 0, 0, t).wait()
            project((i == 0) & (t < 2), t, 1, 4 + t % 2, jnp.where(t < 2, core, 1 - core) * NH + i)
            return 0

        lax.fori_loop(0, 4, step, 0)
        return 0

    lax.fori_loop(0, NCH - NH, window2, 0)
    ostore(0, 0, 0).wait()
    ostore(0, 0, 1).wait()

    def drain(ch, _):
        y(ch).wait_send()
        s0(ch).wait_send()
        s1(ch).wait_send()

        @pl.when(diag)
        def _():
            p(ch).wait_send()

        @pl.when(diag | (ch >= NH))
        def _():
            q_hop(ch).wait_send()
        return 0

    lax.fori_loop(0, NCH, drain, 0)


def last_back_kernel(a0, a1, b0, b1, z_ref, x_ref, gate_ref, gain_ref, proj_ref, first_ref, o_ref, gate_t, gain, proj_t, o_scr):
    step = pl.program_id(0)

    @pl.when(step == 0)
    def _():
        out_weights(gate_ref, gain_ref, proj_ref, gate_t, gain, proj_t)

    @pl.when(step >= N_C)
    def _():
        o_ref[:, :, :HALF] = first_ref[...]
    back_body(step, a0, a1, b0, b1, z_ref, x_ref, o_ref, gate_t, gain, proj_t, o_scr)


def solution(mesh):
    tile_spec = P(('batch', 'row'), 'col', None)
    mask_spec = P(('batch', 'row'), 'col')
    repl_spec = P()
    any_spec = pl.BlockSpec(memory_space=pl.ANY)
    vmem_spec = pl.BlockSpec(memory_space=pltpu.VMEM)
    dma = pltpu.SemaphoreType.DMA

    def per_device(z_tile, mask_tile, ln_in_gain, proj_a, gate_a, proj_b, gate_b, gate_out, proj_out, ln_out_gain):
        gain_in, gain_out = ln_in_gain.reshape(1, PAIR), ln_out_gain.reshape(HID // LANES, LANES)
        z4 = z_tile.reshape(ROWS, 2, 2 * HALF, PAIR)
        out_w = [pltpu.VMEM((PAIR, PAIR), BF16), pltpu.VMEM((HID, 1), F32), pltpu.VMEM((PAIR, HID), BF16)]

        _, g, xt, first = pl.pallas_call(
            main_kernel,
            out_shape=(
                jax.ShapeDtypeStruct((2, 3, ROWS, PAIR, COLS), BF16),
                jax.ShapeDtypeStruct((6, HID, ROWS, COLS), BF16),
                jax.ShapeDtypeStruct((ROWS, PAIR, COLS), BF16),
                jax.ShapeDtypeStruct((ROWS, 2, HALF, PAIR), BF16),
            ),
            in_specs=[any_spec, any_spec] + [vmem_spec] * 9,
            out_specs=(any_spec,) * 4,
            scratch_shapes=[
                pltpu.VMEM((ROWS, COLS), jnp.int32),
                pltpu.VMEM((2, 2 * HID, PAIR), BF16),
                *out_w,
                pltpu.VMEM((2, FB, COLS, PAIR), BF16),
                pltpu.VMEM((2, FB, PAIR, COLS), BF16),
                pltpu.VMEM((2, FB, PAIR, COLS), BF16),
                pltpu.VMEM((4, FB, PAIR, COLS), BF16),
                pltpu.VMEM((2, HID, FB, COLS), BF16),
                pltpu.VMEM((COLS // LANES, FB * PITCH, LANES), F32),
                pltpu.VMEM((HID * OPITCH, 2 * HALF), F32),
                dma((2,)), dma((2,)), dma((2,)), dma((4,)), dma((2,)),
            ] + [dma((NCH,))] * 10,
            compiler_params=pltpu.CompilerParams(vmem_limit_bytes=VMEM_LIMIT, collective_id=0, has_side_effects=True),
            name='exchange_project',
        )(z_tile, z4, mask_tile, gain_in, proj_a, gate_a, proj_b, gate_b, gate_out, gain_out, proj_out)

        def whole(*shape):
            return pl.BlockSpec(shape, lambda s: (0,) * len(shape))

        specs, first_spec = back_specs(1)
        out = pl.pallas_call(
            last_back_kernel,
            grid=(N_C + N_I,),
            out_shape=jax.ShapeDtypeStruct((ROWS, 2, 2 * HALF, PAIR), BF16),
            in_specs=specs + [whole(PAIR, PAIR), whole(HID // LANES, LANES), whole(HID, PAIR), first_spec],
            out_specs=pl.BlockSpec((IB, 2, 2 * HALF, PAIR), lambda s: (jnp.maximum(s - N_C, 0), 0, 0, 0)),
            scratch_shapes=[*out_w, pltpu.VMEM((HID * OPITCH, 2 * HALF), F32)],
            compiler_params=pltpu.CompilerParams(vmem_limit_bytes=VMEM_LIMIT),
            name='back',
        )(g, g, g, g, z4, xt, gate_out, gain_out, proj_out, first)
        return out.reshape(ROWS, COLS, PAIR)

    return jax.shard_map(per_device, mesh=mesh, in_specs=(tile_spec, mask_spec) + (repl_spec,) * 8, out_specs=tile_spec, check_vma=False)
```

```python
import jax
import jax.numpy as jnp
from jax import lax
from jax.experimental import pallas as pl
from jax.experimental.pallas import tpu as pltpu
from jax.sharding import PartitionSpec as P

LN_EPS = 1e-5
F32 = jnp.float32
BF16 = jnp.bfloat16
VMEM_LIMIT = 60 * 1024 * 1024
MESH = pl.DeviceIdType.MESH

ROWS, COLS, PAIR, HID = 128, 256, 128, 256
HALF = ROWS // 2
LANES = 128
FB = 16
NCH = ROWS // FB
LAST = NCH - 1
NH = NCH // 2
CH = 128
PITCH = HID + 4
OPITCH = ROWS + 4
CB = 32
IB = 32
N_C, N_I = HID // CB, ROWS // IB


def normed_t(v, gain):
    mean = jnp.mean(v, axis=0, keepdims=True)
    cen = v - mean
    var = jnp.mean(cen * cen, axis=0, keepdims=True)
    return cen * lax.rsqrt(var + LN_EPS) * gain


def norm_chunk(z_ref, m_ref, first, gain, x_ref, xm_ref):
    for r in range(FB):
        z = z_ref[r].reshape(2, 2, HALF, PAIR)
        z = jnp.concatenate([z[0, 0], z[1, 0], z[0, 1], z[1, 1]], axis=0)
        x = normed_t(z.astype(F32).T, gain)
        x_ref[r] = x.astype(BF16)
        xm_ref[r] = (x * m_ref[pl.ds(first + r, 1), :].astype(F32)).astype(BF16)


def project_rows(x_ref, w_ref, rows, scr, base):
    for r in rows:
        x = x_ref[r]
        for c in range(0, HID, CH):
            both = jnp.dot(w_ref[2 * c:2 * (c + CH), :], x, preferred_element_type=F32)
            proj = both[:CH]
            val = proj + jnp.tanh(both[CH:]) * proj
            for n in range(COLS // LANES):
                scr[pl.ds(base[n] + r * PITCH + c, CH), :] = val[:, n * LANES:(n + 1) * LANES]


def write_channels(o_ref, scr, base):
    def channel(c, _):
        for n in range(COLS // LANES):
            o_ref[c, :, n * LANES:(n + 1) * LANES] = scr[pl.ds(base[n] + c, FB, stride=PITCH), :].astype(BF16)
        return 0

    lax.fori_loop(0, HID, channel, 0, unroll=16)


def bases(t):
    return [(t * (COLS // LANES) + n) * FB * PITCH for n in range(COLS // LANES)]


def column(row_ref):
    cols = row_ref[...].astype(F32).T
    return jnp.concatenate([cols[:, n:n + 1] for n in range(cols.shape[1])], axis=0)


def out_weights(gate_ref, gain_ref, proj_ref, gate_t, gain, proj_t):
    gate_t[...] = (gate_ref[...].astype(F32).T * 0.5).astype(BF16)
    gain[...] = column(gain_ref)
    proj_t[...] = (proj_ref[...].astype(F32).T * 0.5).astype(BF16)


def back_body(step, a0, a1, b0, b1, z_ref, x_ref, o_ref, gate_ref, gain_ref, proj_ref, o_scr):
    @pl.when(step < N_C)
    def _():
        for c in range(CB):
            dims = (((1,), (1,)), ((), ()))
            acc = lax.dot_general(a0[0, c], b0[0, c], dims, preferred_element_type=F32)
            acc = acc + lax.dot_general(a1[0, c], b1[0, c], dims, preferred_element_type=F32)
            o_scr[pl.ds(pl.multiple_of((step * CB + c) * OPITCH, 4), ROWS), :] = acc

    @pl.when(step >= N_C)
    def _():
        first = (step - N_C) * IB
        gain = gain_ref[...]

        def one_row(i, _):
            tri = o_scr[pl.ds(first + i, HID, stride=OPITCH), :]
            y = normed_t(tri, gain).astype(BF16)
            u = jnp.dot(proj_ref[...], y, preferred_element_type=F32)
            t = jnp.tanh(jnp.dot(gate_ref[...], x_ref[i], preferred_element_type=F32))
            z = z_ref[i].reshape(2 * HALF, PAIR).astype(F32)
            o_ref[i, :, o_ref.shape[2] - HALF:] = (z + (u + t * u).T).astype(BF16).reshape(2, HALF, PAIR)
            return 0

        lax.fori_loop(0, IB, one_row, 0, unroll=32)


def back_specs(half):
    def chan(slot):
        return pl.BlockSpec((1, CB, ROWS, COLS), lambda s: (slot, jnp.minimum(s, N_C - 1), 0, 0))

    tile = pl.BlockSpec((IB, 2, HALF, PAIR), lambda s: (jnp.maximum(s - N_C, 0), 0, half, 0))
    first = pl.BlockSpec((IB, 2, HALF, PAIR), lambda s: (jnp.maximum(s - N_C, 0), 0, 0, 0))
    x_spec = pl.BlockSpec((IB, PAIR, 2 * HALF), lambda s: (jnp.maximum(s - N_C, 0), 0, half))
    return [chan(0), chan(1), chan(2 + 2 * half), chan(3 + 2 * half), tile, x_spec], first


def main_kernel(z_ref, z4_ref, mask_in, gain_in, proj_a, gate_a, proj_b, gate_b, gate_in, gout_in, proj_in,
                xb, g_ref, xt, out_ref,
                mask_ref, w_ref, gate_ref, gout_ref, proj_ref, zbuf, xubuf, xmbuf, xin, obuf, scr, o_scr,
                zsem, xusem, xmsem, xsem, osem,
                y_s, p_s, q_s, s0_s, s1_s, y_r, p_r, q_r, s0_r, s1_r):
    row, col = lax.axis_index('row'), lax.axis_index('col')
    chip, core = row // 2, row % 2
    ydev = {'col': 1 - col}
    xdev = {'row': (1 - chip) * 2 + core}
    sdev = {'row': chip * 2 + 1 - core}
    diag = chip == col
    off = chip != col
    mine = 1 - diag.astype(jnp.int32)

    def part(k, slot, ch):
        return xb.at[k, slot, pl.ds(ch * FB, FB)]

    def rdma(src, dst, send, recv, dev):
        return pltpu.make_async_remote_copy(src_ref=src, dst_ref=dst, send_sem=send, recv_sem=recv,
                                            device_id=dev, device_id_type=MESH)

    def piece(k, slot, n):
        return xb.at[k, slot, pl.ds(LAST * FB + n * FB // 2, FB // 2)]

    def p_piece(n):
        return rdma(piece(0, 0, n), piece(0, 1, n), p_s.at[LAST + n], p_r.at[LAST + n], xdev)

    def q_piece(n):
        return rdma(piece(1, 1, n), piece(1, 1, n), q_s.at[LAST + n], q_r.at[LAST + n], ydev)

    def s0_piece(n):
        return rdma(piece(0, mine, n), piece(0, 2, n), s0_s.at[LAST + n], s0_r.at[LAST + n], sdev)

    def s1_piece(n):
        return rdma(piece(1, mine, n), piece(1, 2, n), s1_s.at[LAST + n], s1_r.at[LAST + n], sdev)

    def y(ch):
        return rdma(part(0, 0, ch), part(1, 0, ch), y_s.at[ch], y_r.at[ch], ydev)

    def p(ch):
        return rdma(part(0, 0, ch), part(0, 1, ch), p_s.at[ch], p_r.at[ch], xdev)

    def q_relay(ch):
        return rdma(part(1, 0, ch), part(1, 1, ch), q_s.at[ch], q_r.at[ch], xdev)

    def q_hop(ch):
        return rdma(part(0, 0, ch), part(1, 1, ch), q_s.at[ch], q_r.at[ch], xdev)

    def q_hop2(ch):
        return rdma(part(1, 1, ch), part(1, 1, ch), q_s.at[ch], q_r.at[ch], ydev)

    def s0(ch):
        return rdma(part(0, mine, ch), part(0, 2, ch), s0_s.at[ch], s0_r.at[ch], sdev)

    def s1(ch):
        return rdma(part(1, mine, ch), part(1, 2, ch), s1_s.at[ch], s1_r.at[ch], sdev)

    barrier = pltpu.get_barrier_semaphore()
    for dev in (ydev, xdev, sdev):
        pl.semaphore_signal(barrier, inc=1, device_id=dev, device_id_type=MESH)

    def zload(ch):
        return pltpu.make_async_copy(z_ref.at[pl.ds(ch * FB, FB)], zbuf.at[ch % 2], zsem.at[ch % 2])

    def xustore(ch):
        return pltpu.make_async_copy(xubuf.at[ch % 2], xt.at[pl.ds(ch * FB, FB)], xusem.at[ch % 2])

    def xmstore(ch):
        return pltpu.make_async_copy(xmbuf.at[ch % 2], part(0, 0, ch), xmsem.at[ch % 2])

    def publish(ch):
        xmstore(ch).wait()
        y(ch).start()

        @pl.when(diag & (ch < LAST))
        def _():
            s0(ch).start()

        @pl.when(diag & (ch == LAST))
        def _():
            for n in range(2):
                s0_piece(n).start()

        @pl.when(diag & (ch < NH))
        def _():
            p(ch).start()

        @pl.when(off & (ch >= NH))
        def _():
            q_hop(ch).start()

    zload(0).start()
    gain = column(gain_in)
    mask = mask_in[...]
    mask_ref[...] = jnp.concatenate([mask[:, n * HALF:(n + 1) * HALF] for n in (0, 2, 1, 3)], axis=1)
    pl.semaphore_wait(barrier, 3)

    def norm_step(ch, _):
        @pl.when(ch + 1 < NCH)
        def _():
            zload(ch + 1).start()

        @pl.when(ch >= 2)
        def _():
            xustore(ch - 2).wait()

        zload(ch).wait()
        norm_chunk(zbuf.at[ch % 2], mask_ref, ch * FB, gain, xubuf.at[ch % 2], xmbuf.at[ch % 2])
        xustore(ch).start()
        xmstore(ch).start()

        @pl.when(ch == 0)
        def _():
            publish(0)

        @pl.when(ch >= 2)
        def _():
            publish(ch - 1)
        return 0

    lax.fori_loop(0, NCH, norm_step, 0)
    publish(NCH - 1)
    xustore(NCH - 2).wait()
    xustore(NCH - 1).wait()

    for n, (proj, gate) in enumerate(((proj_a, gate_a), (proj_b, gate_b))):
        for half, ref in ((0, proj), (1, gate)):
            w_t = (ref[...].astype(F32).T * 0.5).astype(BF16)
            for c in range(HID // CH):
                w_ref[n, pl.ds((2 * c + half) * CH, CH), :] = w_t[c * CH:(c + 1) * CH]
    out_weights(gate_in, gout_in, proj_in, gate_ref, gout_ref, proj_ref)

    def xload(k, slot, ch, t):
        return pltpu.make_async_copy(part(k, slot, ch), xin.at[t], xsem.at[t])

    def ostore(dst, block, t):
        return pltpu.make_async_copy(obuf.at[t % 2], g_ref.at[dst, :, pl.ds(block * FB, FB), :], osem.at[t % 2])

    def project(first_use, t, weight, dst, block):
        @pl.when(jnp.logical_not(first_use))
        def _():
            ostore(0, 0, t).wait()
        project_rows(xin.at[t], w_ref.at[weight], range(FB), scr, bases(0))
        write_channels(obuf.at[t % 2], scr, bases(0))
        ostore(dst, block, t).start()

    def window1(i, _):
        k, ch = i // NH, i % NH
        y(i).wait_recv()

        @pl.when(diag & (i < LAST))
        def _():
            s1(i).start()

        @pl.when(diag & (i == LAST))
        def _():
            for n in range(2):
                s1_piece(n).start()

        @pl.when(diag & (i < NH))
        def _():
            q_relay(i).start()

        @pl.when(diag & (i == NH - 1))
        def _():
            for c in range(NH, LAST):
                p(c).start()
            for n in range(2):
                p_piece(n).start()

        @pl.when(diag & (i >= NH))
        def _():
            q_hop(i).wait_recv()

        @pl.when(diag & (i >= NH) & (i < LAST))
        def _():
            q_hop2(i).start()

        @pl.when(diag & (i == LAST))
        def _():
            for n in range(2):
                q_piece(n).start()

        @pl.when(off & (i < NH))
        def _():
            p(ch).wait_recv()
            s0(ch).start()

        @pl.when(off & (i >= NH))
        def _():
            q_relay(ch).wait_recv()
            s1(ch).start()

        xload(0, 0, i, 0).start()
        xload(1, 0, i, 1).start()
        xload(k, mine, ch, 2).start()

        def step(t, _):
            @pl.when((t == 1) & (i < NH))
            def _():
                s0(ch).wait_recv()

            @pl.when((t == 1) & (i >= NH))
            def _():
                s1(ch).wait_recv()

            @pl.when(t == 1)
            def _():
                xload(k, 2, ch, 3).start()

            xload(0, 0, 0, t).wait()
            is_b = t // 2
            own_block = jnp.where(t == 2, core, 1 - core) * NH + ch
            project((i == 0) & (t < 2), t, is_b, jnp.where(is_b == 1, 2 + k, t), jnp.where(is_b == 1, own_block, i))
            return 0

        lax.fori_loop(0, 4, step, 0)
        return 0

    lax.fori_loop(0, NCH, window1, 0)
    ostore(0, 0, 0).wait()
    ostore(0, 0, 1).wait()

    specs, out_spec = back_specs(0)

    def pipe(a0, a1, b0, b1, zr, xr, o):
        back_body(pl.program_id(0), a0, a1, b0, b1, zr, xr, o, gate_ref, gout_ref, proj_ref, o_scr)

    pltpu.emit_pipeline(pipe, grid=(N_C + N_I,), in_specs=specs, out_specs=[out_spec])(
        g_ref, g_ref, g_ref, g_ref, z4_ref, xt, out_ref)

    def window2(i, _):
        ch = NH + i

        @pl.when(off)
        def _():
            p(ch).wait_recv()
            s0(ch).start()
            q_hop2(ch).wait_recv()
            s1(ch).start()

        xload(0, mine, ch, 0).start()
        xload(1, mine, ch, 1).start()

        def step(t, _):
            @pl.when(t == 1)
            def _():
                s0(ch).wait_recv()
                xload(0, 2, ch, 2).start()
                s1(ch).wait_recv()
                xload(1, 2, ch, 3).start()

            xload(0, 0, 0, t).wait()
            project((i == 0) & (t < 2), t, 1, 4 + t % 2, jnp.where(t < 2, core, 1 - core) * NH + i)
            return 0

        lax.fori_loop(0, 4, step, 0)
        return 0

    lax.fori_loop(0, LAST - NH, window2, 0)

    def xpiece(k, slot, n, t):
        return pltpu.make_async_copy(piece(k, slot, n), xin.at[t, pl.ds(n * FB // 2, FB // 2)], xsem.at[t])

    for n in range(2):
        @pl.when(off)
        def _(n=n):
            p_piece(n).wait_recv()
            s0_piece(n).start()
            q_piece(n).wait_recv()
            s1_piece(n).start()

        xpiece(0, mine, n, 0).start()
        xpiece(1, mine, n, 1).start()
        for t in range(4):
            if t == 1:
                s0_piece(n).wait_recv()
                xpiece(0, 2, n, 2).start()
                s1_piece(n).wait_recv()
                xpiece(1, 2, n, 3).start()
            xpiece(0, 0, n, t).wait()
            project_rows(xin.at[t], w_ref.at[1], range(n * FB // 2, (n + 1) * FB // 2), o_scr, bases(t))
            if n == 1:
                ostore(0, 0, t).wait()
                write_channels(obuf.at[t % 2], o_scr, bases(t))
                ostore(4 + t % 2, (core if t < 2 else 1 - core) * NH + LAST - NH, t).start()
    ostore(0, 0, 0).wait()
    ostore(0, 0, 1).wait()

    def drain(ch, _):
        y(ch).wait_send()

        @pl.when(ch < LAST)
        def _():
            s0(ch).wait_send()
            s1(ch).wait_send()

        @pl.when(diag & (ch < LAST))
        def _():
            p(ch).wait_send()

        @pl.when((diag & (ch < LAST)) | (off & (ch >= NH)))
        def _():
            q_hop(ch).wait_send()
        return 0

    lax.fori_loop(0, NCH, drain, 0)
    for n in range(2):
        s0_piece(n).wait_send()
        s1_piece(n).wait_send()

        @pl.when(diag)
        def _(n=n):
            p_piece(n).wait_send()
            q_piece(n).wait_send()


def last_back_kernel(a0, a1, b0, b1, z_ref, x_ref, gate_ref, gain_ref, proj_ref, first_ref, o_ref, gate_t, gain, proj_t, o_scr):
    step = pl.program_id(0)

    @pl.when(step == 0)
    def _():
        out_weights(gate_ref, gain_ref, proj_ref, gate_t, gain, proj_t)

    @pl.when(step >= N_C)
    def _():
        o_ref[:, :, :HALF] = first_ref[...]
    back_body(step, a0, a1, b0, b1, z_ref, x_ref, o_ref, gate_t, gain, proj_t, o_scr)


def solution(mesh):
    tile_spec = P(('batch', 'row'), 'col', None)
    mask_spec = P(('batch', 'row'), 'col')
    repl_spec = P()
    any_spec = pl.BlockSpec(memory_space=pl.ANY)
    vmem_spec = pl.BlockSpec(memory_space=pltpu.VMEM)
    dma = pltpu.SemaphoreType.DMA

    def per_device(z_tile, mask_tile, ln_in_gain, proj_a, gate_a, proj_b, gate_b, gate_out, proj_out, ln_out_gain):
        gain_in, gain_out = ln_in_gain.reshape(1, PAIR), ln_out_gain.reshape(HID // LANES, LANES)
        z4 = z_tile.reshape(ROWS, 2, 2 * HALF, PAIR)
        out_w = [pltpu.VMEM((PAIR, PAIR), BF16), pltpu.VMEM((HID, 1), F32), pltpu.VMEM((PAIR, HID), BF16)]

        _, g, xt, first = pl.pallas_call(
            main_kernel,
            out_shape=(
                jax.ShapeDtypeStruct((2, 3, ROWS, PAIR, COLS), BF16),
                jax.ShapeDtypeStruct((6, HID, ROWS, COLS), BF16),
                jax.ShapeDtypeStruct((ROWS, PAIR, COLS), BF16),
                jax.ShapeDtypeStruct((ROWS, 2, HALF, PAIR), BF16),
            ),
            in_specs=[any_spec, any_spec] + [vmem_spec] * 9,
            out_specs=(any_spec,) * 4,
            scratch_shapes=[
                pltpu.VMEM((ROWS, COLS), jnp.int32),
                pltpu.VMEM((2, 2 * HID, PAIR), BF16),
                *out_w,
                pltpu.VMEM((2, FB, COLS, PAIR), BF16),
                pltpu.VMEM((2, FB, PAIR, COLS), BF16),
                pltpu.VMEM((2, FB, PAIR, COLS), BF16),
                pltpu.VMEM((4, FB, PAIR, COLS), BF16),
                pltpu.VMEM((2, HID, FB, COLS), BF16),
                pltpu.VMEM((COLS // LANES * FB * PITCH, LANES), F32),
                pltpu.VMEM((HID * OPITCH, 2 * HALF), F32),
                dma((2,)), dma((2,)), dma((2,)), dma((4,)), dma((2,)),
            ] + [dma((NCH + 1,))] * 10,
            compiler_params=pltpu.CompilerParams(vmem_limit_bytes=VMEM_LIMIT, collective_id=0, has_side_effects=True),
            name='exchange_project',
        )(z_tile, z4, mask_tile, gain_in, proj_a, gate_a, proj_b, gate_b, gate_out, gain_out, proj_out)

        def whole(*shape):
            return pl.BlockSpec(shape, lambda s: (0,) * len(shape))

        specs, first_spec = back_specs(1)
        out = pl.pallas_call(
            last_back_kernel,
            grid=(N_C + N_I,),
            out_shape=jax.ShapeDtypeStruct((ROWS, 2, 2 * HALF, PAIR), BF16),
            in_specs=specs + [whole(PAIR, PAIR), whole(HID // LANES, LANES), whole(HID, PAIR), first_spec],
            out_specs=pl.BlockSpec((IB, 2, 2 * HALF, PAIR), lambda s: (jnp.maximum(s - N_C, 0), 0, 0, 0)),
            scratch_shapes=[*out_w, pltpu.VMEM((HID * OPITCH, 2 * HALF), F32)],
            compiler_params=pltpu.CompilerParams(vmem_limit_bytes=VMEM_LIMIT),
            name='back',
        )(g, g, g, g, z4, xt, gate_out, gain_out, proj_out, first)
        return out.reshape(ROWS, COLS, PAIR)

    return jax.shard_map(per_device, mesh=mesh, in_specs=(tile_spec, mask_spec) + (repl_spec,) * 8, out_specs=tile_spec, check_vma=False)
```

```python
import jax
import jax.numpy as jnp
from jax import lax
from jax.experimental import pallas as pl
from jax.experimental.pallas import tpu as pltpu
from jax.sharding import PartitionSpec as P

LN_EPS = 1e-5
F32 = jnp.float32
BF16 = jnp.bfloat16
VMEM_LIMIT = 60 * 1024 * 1024
MESH = pl.DeviceIdType.MESH

ROWS, COLS, PAIR, HID = 128, 256, 128, 256
HALF = ROWS // 2
LANES = 128
FB = 16
NCH = ROWS // FB
LAST = NCH - 1
PIECES = (0, 8, 12, 16)
N_P = len(PIECES) - 1
NH = NCH // 2
CH = 128
PITCH = HID + 4
OPITCH = ROWS + 4
CB = 32
IB = 32
N_C, N_I = HID // CB, ROWS // IB


def normed_t(v, gain):
    mean = jnp.mean(v, axis=0, keepdims=True)
    cen = v - mean
    var = jnp.mean(cen * cen, axis=0, keepdims=True)
    return cen * lax.rsqrt(var + LN_EPS) * gain


def norm_chunk(z_ref, m_ref, first, gain, x_ref, xm_ref):
    for r in range(FB):
        z = z_ref[r].reshape(2, 2, HALF, PAIR)
        z = jnp.concatenate([z[0, 0], z[1, 0], z[0, 1], z[1, 1]], axis=0)
        x = normed_t(z.astype(F32).T, gain)
        x_ref[r] = x.astype(BF16)
        xm_ref[r] = (x * m_ref[pl.ds(first + r, 1), :].astype(F32)).astype(BF16)


def project_rows(x_ref, w_ref, rows, scr, base):
    for r in rows:
        x = x_ref[r]
        for c in range(0, HID, CH):
            both = jnp.dot(w_ref[2 * c:2 * (c + CH), :], x, preferred_element_type=F32)
            proj = both[:CH]
            val = proj + jnp.tanh(both[CH:]) * proj
            for n in range(COLS // LANES):
                scr[pl.ds(base[n] + r * PITCH + c, CH), :] = val[:, n * LANES:(n + 1) * LANES]


def write_channels(o_ref, scr, base):
    def channel(c, _):
        for n in range(COLS // LANES):
            o_ref[c, :, n * LANES:(n + 1) * LANES] = scr[pl.ds(base[n] + c, FB, stride=PITCH), :].astype(BF16)
        return 0

    lax.fori_loop(0, HID, channel, 0, unroll=16)


def bases(t):
    return [(t * (COLS // LANES) + n) * FB * PITCH for n in range(COLS // LANES)]


def column(row_ref):
    cols = row_ref[...].astype(F32).T
    return jnp.concatenate([cols[:, n:n + 1] for n in range(cols.shape[1])], axis=0)


def out_weights(gate_ref, gain_ref, proj_ref, gate_t, gain, proj_t):
    gate_t[...] = (gate_ref[...].astype(F32).T * 0.5).astype(BF16)
    gain[...] = column(gain_ref)
    proj_t[...] = (proj_ref[...].astype(F32).T * 0.5).astype(BF16)


def back_body(step, a0, a1, b0, b1, z_ref, x_ref, o_ref, gate_ref, gain_ref, proj_ref, o_scr):
    @pl.when(step < N_C)
    def _():
        for c in range(CB):
            dims = (((1,), (1,)), ((), ()))
            acc = lax.dot_general(a0[0, c], b0[0, c], dims, preferred_element_type=F32)
            acc = acc + lax.dot_general(a1[0, c], b1[0, c], dims, preferred_element_type=F32)
            o_scr[pl.ds(pl.multiple_of((step * CB + c) * OPITCH, 4), ROWS), :] = acc

    @pl.when(step >= N_C)
    def _():
        first = (step - N_C) * IB
        gain = gain_ref[...]

        def one_row(i, _):
            tri = o_scr[pl.ds(first + i, HID, stride=OPITCH), :]
            y = normed_t(tri, gain).astype(BF16)
            u = jnp.dot(proj_ref[...], y, preferred_element_type=F32)
            t = jnp.tanh(jnp.dot(gate_ref[...], x_ref[i], preferred_element_type=F32))
            z = z_ref[i].reshape(2 * HALF, PAIR).astype(F32)
            o_ref[i, :, o_ref.shape[2] - HALF:] = (z + (u + t * u).T).astype(BF16).reshape(2, HALF, PAIR)
            return 0

        lax.fori_loop(0, IB, one_row, 0, unroll=32)


def back_specs(half):
    def chan(slot):
        return pl.BlockSpec((1, CB, ROWS, COLS), lambda s: (slot, jnp.minimum(s, N_C - 1), 0, 0))

    tile = pl.BlockSpec((IB, 2, HALF, PAIR), lambda s: (jnp.maximum(s - N_C, 0), 0, half, 0))
    first = pl.BlockSpec((IB, 2, HALF, PAIR), lambda s: (jnp.maximum(s - N_C, 0), 0, 0, 0))
    x_spec = pl.BlockSpec((IB, PAIR, 2 * HALF), lambda s: (jnp.maximum(s - N_C, 0), 0, half))
    return [chan(0), chan(1), chan(2 + 2 * half), chan(3 + 2 * half), tile, x_spec], first


def main_kernel(z_ref, z4_ref, mask_in, gain_in, proj_a, gate_a, proj_b, gate_b, gate_in, gout_in, proj_in,
                xb, g_ref, xt, out_ref,
                mask_ref, w_ref, gate_ref, gout_ref, proj_ref, zbuf, xubuf, xmbuf, xin, obuf, scr, o_scr,
                zsem, xusem, xmsem, xsem, osem,
                y_s, p_s, q_s, s0_s, s1_s, y_r, p_r, q_r, s0_r, s1_r):
    row, col = lax.axis_index('row'), lax.axis_index('col')
    chip, core = row // 2, row % 2
    ydev = {'col': 1 - col}
    xdev = {'row': (1 - chip) * 2 + core}
    sdev = {'row': chip * 2 + 1 - core}
    diag = chip == col
    off = chip != col
    mine = 1 - diag.astype(jnp.int32)

    def part(k, slot, ch):
        return xb.at[k, slot, pl.ds(ch * FB, FB)]

    def rdma(src, dst, send, recv, dev):
        return pltpu.make_async_remote_copy(src_ref=src, dst_ref=dst, send_sem=send, recv_sem=recv,
                                            device_id=dev, device_id_type=MESH)

    def piece(k, slot, n):
        return xb.at[k, slot, pl.ds(LAST * FB + PIECES[n], PIECES[n + 1] - PIECES[n])]

    def p_piece(n):
        return rdma(piece(0, 0, n), piece(0, 1, n), p_s.at[LAST + n], p_r.at[LAST + n], xdev)

    def q_piece(n):
        return rdma(piece(1, 1, n), piece(1, 1, n), q_s.at[LAST + n], q_r.at[LAST + n], ydev)

    def s0_piece(n):
        return rdma(piece(0, mine, n), piece(0, 2, n), s0_s.at[LAST + n], s0_r.at[LAST + n], sdev)

    def s1_piece(n):
        return rdma(piece(1, mine, n), piece(1, 2, n), s1_s.at[LAST + n], s1_r.at[LAST + n], sdev)

    def y(ch):
        return rdma(part(0, 0, ch), part(1, 0, ch), y_s.at[ch], y_r.at[ch], ydev)

    def p(ch):
        return rdma(part(0, 0, ch), part(0, 1, ch), p_s.at[ch], p_r.at[ch], xdev)

    def q_relay(ch):
        return rdma(part(1, 0, ch), part(1, 1, ch), q_s.at[ch], q_r.at[ch], xdev)

    def q_hop(ch):
        return rdma(part(0, 0, ch), part(1, 1, ch), q_s.at[ch], q_r.at[ch], xdev)

    def q_hop2(ch):
        return rdma(part(1, 1, ch), part(1, 1, ch), q_s.at[ch], q_r.at[ch], ydev)

    def s0(ch):
        return rdma(part(0, mine, ch), part(0, 2, ch), s0_s.at[ch], s0_r.at[ch], sdev)

    def s1(ch):
        return rdma(part(1, mine, ch), part(1, 2, ch), s1_s.at[ch], s1_r.at[ch], sdev)

    barrier = pltpu.get_barrier_semaphore()
    for dev in (ydev, xdev, sdev):
        pl.semaphore_signal(barrier, inc=1, device_id=dev, device_id_type=MESH)

    def zload(ch):
        return pltpu.make_async_copy(z_ref.at[pl.ds(ch * FB, FB)], zbuf.at[ch % 2], zsem.at[ch % 2])

    def xustore(ch):
        return pltpu.make_async_copy(xubuf.at[ch % 2], xt.at[pl.ds(ch * FB, FB)], xusem.at[ch % 2])

    def xmstore(ch):
        return pltpu.make_async_copy(xmbuf.at[ch % 2], part(0, 0, ch), xmsem.at[ch % 2])

    def publish(ch):
        xmstore(ch).wait()
        y(ch).start()

        @pl.when(diag & (ch < LAST))
        def _():
            s0(ch).start()

        @pl.when(diag & (ch == LAST))
        def _():
            for n in range(N_P):
                s0_piece(n).start()

        @pl.when(diag & (ch < NH))
        def _():
            p(ch).start()

        @pl.when(off & (ch >= NH))
        def _():
            q_hop(ch).start()

    zload(0).start()
    gain = column(gain_in)
    mask = mask_in[...]
    mask_ref[...] = jnp.concatenate([mask[:, n * HALF:(n + 1) * HALF] for n in (0, 2, 1, 3)], axis=1)

    def norm_step(ch, _):
        @pl.when(ch + 1 < NCH)
        def _():
            zload(ch + 1).start()

        @pl.when(ch >= 2)
        def _():
            xustore(ch - 2).wait()

        zload(ch).wait()
        norm_chunk(zbuf.at[ch % 2], mask_ref, ch * FB, gain, xubuf.at[ch % 2], xmbuf.at[ch % 2])
        xustore(ch).start()
        xmstore(ch).start()

        @pl.when(ch == 0)
        def _():
            pl.semaphore_wait(barrier, 3)
            publish(0)

        @pl.when(ch >= 2)
        def _():
            publish(ch - 1)
        return 0

    lax.fori_loop(0, NCH, norm_step, 0)
    publish(NCH - 1)
    xustore(NCH - 2).wait()
    xustore(NCH - 1).wait()

    for n, (proj, gate) in enumerate(((proj_a, gate_a), (proj_b, gate_b))):
        for half, ref in ((0, proj), (1, gate)):
            w_t = (ref[...].astype(F32).T * 0.5).astype(BF16)
            for c in range(HID // CH):
                w_ref[n, pl.ds((2 * c + half) * CH, CH), :] = w_t[c * CH:(c + 1) * CH]
    out_weights(gate_in, gout_in, proj_in, gate_ref, gout_ref, proj_ref)

    def xload(k, slot, ch, t):
        return pltpu.make_async_copy(part(k, slot, ch), xin.at[t], xsem.at[t])

    def ostore(dst, block, t):
        return pltpu.make_async_copy(obuf.at[t % 2], g_ref.at[dst, :, pl.ds(block * FB, FB), :], osem.at[t % 2])

    def project(first_use, t, weight, dst, block):
        @pl.when(jnp.logical_not(first_use))
        def _():
            ostore(0, 0, t).wait()
        project_rows(xin.at[t], w_ref.at[weight], range(FB), scr, bases(0))
        write_channels(obuf.at[t % 2], scr, bases(0))
        ostore(dst, block, t).start()

    def window1(i, _):
        k, ch = i // NH, i % NH
        y(i).wait_recv()

        @pl.when(diag & (i < LAST))
        def _():
            s1(i).start()

        @pl.when(diag & (i == LAST))
        def _():
            for n in range(N_P):
                s1_piece(n).start()

        @pl.when(diag & (i < NH))
        def _():
            q_relay(i).start()

        @pl.when(diag & (i == NH - 1))
        def _():
            for c in range(NH, LAST):
                p(c).start()
            for n in range(N_P):
                p_piece(n).start()

        @pl.when(diag & (i >= NH))
        def _():
            q_hop(i).wait_recv()

        @pl.when(diag & (i >= NH) & (i < LAST))
        def _():
            q_hop2(i).start()

        @pl.when(diag & (i == LAST))
        def _():
            for n in range(N_P):
                q_piece(n).start()

        @pl.when(off & (i < NH))
        def _():
            p(ch).wait_recv()
            s0(ch).start()

        @pl.when(off & (i >= NH))
        def _():
            q_relay(ch).wait_recv()
            s1(ch).start()

        xload(0, 0, i, 0).start()
        xload(1, 0, i, 1).start()
        xload(k, mine, ch, 2).start()

        def step(t, _):
            @pl.when((t == 1) & (i < NH))
            def _():
                s0(ch).wait_recv()

            @pl.when((t == 1) & (i >= NH))
            def _():
                s1(ch).wait_recv()

            @pl.when(t == 1)
            def _():
                xload(k, 2, ch, 3).start()

            xload(0, 0, 0, t).wait()
            is_b = t // 2
            own_block = jnp.where(t == 2, core, 1 - core) * NH + ch
            project((i == 0) & (t < 2), t, is_b, jnp.where(is_b == 1, 2 + k, t), jnp.where(is_b == 1, own_block, i))
            return 0

        lax.fori_loop(0, 4, step, 0)
        return 0

    lax.fori_loop(0, NCH, window1, 0)
    ostore(0, 0, 0).wait()
    ostore(0, 0, 1).wait()

    specs, out_spec = back_specs(0)

    def pipe(a0, a1, b0, b1, zr, xr, o):
        back_body(pl.program_id(0), a0, a1, b0, b1, zr, xr, o, gate_ref, gout_ref, proj_ref, o_scr)

    pltpu.emit_pipeline(pipe, grid=(N_C + N_I,), in_specs=specs, out_specs=[out_spec])(
        g_ref, g_ref, g_ref, g_ref, z4_ref, xt, out_ref)

    def window2(i, _):
        ch = NH + i

        @pl.when(off)
        def _():
            p(ch).wait_recv()
            s0(ch).start()
            q_hop2(ch).wait_recv()
            s1(ch).start()

        xload(0, mine, ch, 0).start()
        xload(1, mine, ch, 1).start()

        def step(t, _):
            @pl.when(t == 1)
            def _():
                s0(ch).wait_recv()
                xload(0, 2, ch, 2).start()
                s1(ch).wait_recv()
                xload(1, 2, ch, 3).start()

            xload(0, 0, 0, t).wait()
            project((i == 0) & (t < 2), t, 1, 4 + t % 2, jnp.where(t < 2, core, 1 - core) * NH + i)
            return 0

        lax.fori_loop(0, 4, step, 0)
        return 0

    lax.fori_loop(0, LAST - NH, window2, 0)

    def xpiece(k, slot, n, t):
        return pltpu.make_async_copy(piece(k, slot, n), xin.at[t, pl.ds(PIECES[n], PIECES[n + 1] - PIECES[n])], xsem.at[t])

    for n in range(N_P):
        @pl.when(off)
        def _(n=n):
            p_piece(n).wait_recv()
            s0_piece(n).start()

        xpiece(0, mine, n, 0).start()

        @pl.when(off)
        def _(n=n):
            q_piece(n).wait_recv()
            s1_piece(n).start()

        xpiece(1, mine, n, 1).start()
        for t in range(4):
            if t == 1:
                s0_piece(n).wait_recv()
                xpiece(0, 2, n, 2).start()
                s1_piece(n).wait_recv()
                xpiece(1, 2, n, 3).start()
            xpiece(0, 0, n, t).wait()
            project_rows(xin.at[t], w_ref.at[1], range(PIECES[n], PIECES[n + 1]), o_scr, bases(t))
            if n == N_P - 1:
                ostore(0, 0, t).wait()
                write_channels(obuf.at[t % 2], o_scr, bases(t))
                ostore(4 + t % 2, (core if t < 2 else 1 - core) * NH + LAST - NH, t).start()
    ostore(0, 0, 0).wait()
    ostore(0, 0, 1).wait()

    def drain(ch, _):
        y(ch).wait_send()

        @pl.when(ch < LAST)
        def _():
            s0(ch).wait_send()
            s1(ch).wait_send()

        @pl.when(diag & (ch < LAST))
        def _():
            p(ch).wait_send()

        @pl.when((diag & (ch < LAST)) | (off & (ch >= NH)))
        def _():
            q_hop(ch).wait_send()
        return 0

    lax.fori_loop(0, NCH, drain, 0)
    for n in range(N_P):
        s0_piece(n).wait_send()
        s1_piece(n).wait_send()

        @pl.when(diag)
        def _(n=n):
            p_piece(n).wait_send()
            q_piece(n).wait_send()


def last_back_kernel(a0, a1, b0, b1, z_ref, x_ref, gate_ref, gain_ref, proj_ref, first_ref, o_ref, gate_t, gain, proj_t, o_scr):
    step = pl.program_id(0)

    @pl.when(step == 0)
    def _():
        out_weights(gate_ref, gain_ref, proj_ref, gate_t, gain, proj_t)

    @pl.when(step >= N_C)
    def _():
        o_ref[:, :, :HALF] = first_ref[...]
    back_body(step, a0, a1, b0, b1, z_ref, x_ref, o_ref, gate_t, gain, proj_t, o_scr)


def solution(mesh):
    tile_spec = P(('batch', 'row'), 'col', None)
    mask_spec = P(('batch', 'row'), 'col')
    repl_spec = P()
    any_spec = pl.BlockSpec(memory_space=pl.ANY)
    vmem_spec = pl.BlockSpec(memory_space=pltpu.VMEM)
    dma = pltpu.SemaphoreType.DMA

    def per_device(z_tile, mask_tile, ln_in_gain, proj_a, gate_a, proj_b, gate_b, gate_out, proj_out, ln_out_gain):
        gain_in, gain_out = ln_in_gain.reshape(1, PAIR), ln_out_gain.reshape(HID // LANES, LANES)
        z4 = z_tile.reshape(ROWS, 2, 2 * HALF, PAIR)
        out_w = [pltpu.VMEM((PAIR, PAIR), BF16), pltpu.VMEM((HID, 1), F32), pltpu.VMEM((PAIR, HID), BF16)]

        _, g, xt, first = pl.pallas_call(
            main_kernel,
            out_shape=(
                jax.ShapeDtypeStruct((2, 3, ROWS, PAIR, COLS), BF16),
                jax.ShapeDtypeStruct((6, HID, ROWS, COLS), BF16),
                jax.ShapeDtypeStruct((ROWS, PAIR, COLS), BF16),
                jax.ShapeDtypeStruct((ROWS, 2, HALF, PAIR), BF16),
            ),
            in_specs=[any_spec, any_spec] + [vmem_spec] * 9,
            out_specs=(any_spec,) * 4,
            scratch_shapes=[
                pltpu.VMEM((ROWS, COLS), jnp.int32),
                pltpu.VMEM((2, 2 * HID, PAIR), BF16),
                *out_w,
                pltpu.VMEM((2, FB, COLS, PAIR), BF16),
                pltpu.VMEM((2, FB, PAIR, COLS), BF16),
                pltpu.VMEM((2, FB, PAIR, COLS), BF16),
                pltpu.VMEM((4, FB, PAIR, COLS), BF16),
                pltpu.VMEM((2, HID, FB, COLS), BF16),
                pltpu.VMEM((COLS // LANES * FB * PITCH, LANES), F32),
                pltpu.VMEM((HID * OPITCH, 2 * HALF), F32),
                dma((2,)), dma((2,)), dma((2,)), dma((4,)), dma((2,)),
            ] + [dma((LAST + N_P,))] * 10,
            compiler_params=pltpu.CompilerParams(vmem_limit_bytes=VMEM_LIMIT, collective_id=0, has_side_effects=True),
            name='exchange_project',
        )(z_tile, z4, mask_tile, gain_in, proj_a, gate_a, proj_b, gate_b, gate_out, gain_out, proj_out)

        def whole(*shape):
            return pl.BlockSpec(shape, lambda s: (0,) * len(shape))

        specs, first_spec = back_specs(1)
        out = pl.pallas_call(
            last_back_kernel,
            grid=(N_C + N_I,),
            out_shape=jax.ShapeDtypeStruct((ROWS, 2, 2 * HALF, PAIR), BF16),
            in_specs=specs + [whole(PAIR, PAIR), whole(HID // LANES, LANES), whole(HID, PAIR), first_spec],
            out_specs=pl.BlockSpec((IB, 2, 2 * HALF, PAIR), lambda s: (jnp.maximum(s - N_C, 0), 0, 0, 0)),
            scratch_shapes=[*out_w, pltpu.VMEM((HID * OPITCH, 2 * HALF), F32)],
            compiler_params=pltpu.CompilerParams(vmem_limit_bytes=VMEM_LIMIT),
            name='back',
        )(g, g, g, g, z4, xt, gate_out, gain_out, proj_out, first)
        return out.reshape(ROWS, COLS, PAIR)

    return jax.shard_map(per_device, mesh=mesh, in_specs=(tile_spec, mask_spec) + (repl_spec,) * 8, out_specs=tile_spec, check_vma=False)
```

```python
import jax
import jax.numpy as jnp
from jax import lax
from jax.experimental import pallas as pl
from jax.experimental.pallas import tpu as pltpu
from jax.sharding import PartitionSpec as P

LN_EPS = 1e-5
F32 = jnp.float32
BF16 = jnp.bfloat16
VMEM_LIMIT = 60 * 1024 * 1024
MESH = pl.DeviceIdType.MESH

ROWS, COLS, PAIR, HID = 128, 256, 128, 256
HALF = ROWS // 2
LANES = 128
FB = 16
NCH = ROWS // FB
LAST = NCH - 1
PIECES = (0, 8, 12, 14, 16)
N_P = len(PIECES) - 1
NH = NCH // 2
CH = 128
PITCH = HID + 4
OPITCH = ROWS + 4
CB = 32
IB = 32
N_C, N_I = HID // CB, ROWS // IB


def normed_t(v, gain):
    mean = jnp.mean(v, axis=0, keepdims=True)
    cen = v - mean
    var = jnp.mean(cen * cen, axis=0, keepdims=True)
    return cen * lax.rsqrt(var + LN_EPS) * gain


def norm_chunk(z_ref, m_ref, first, gain, x_ref, xm_ref):
    for r in range(FB):
        z = z_ref[r].reshape(2, 2, HALF, PAIR)
        z = jnp.concatenate([z[0, 0], z[1, 0], z[0, 1], z[1, 1]], axis=0)
        x = normed_t(z.astype(F32).T, gain)
        x_ref[r] = x.astype(BF16)
        xm_ref[r] = (x * m_ref[pl.ds(first + r, 1), :].astype(F32)).astype(BF16)


def project_rows(x_ref, w_ref, rows, scr, base):
    for r in rows:
        x = x_ref[r]
        for c in range(0, HID, CH):
            both = jnp.dot(w_ref[2 * c:2 * (c + CH), :], x, preferred_element_type=F32)
            proj = both[:CH]
            val = proj + jnp.tanh(both[CH:]) * proj
            for n in range(COLS // LANES):
                scr[pl.ds(base[n] + r * PITCH + c, CH), :] = val[:, n * LANES:(n + 1) * LANES]


def write_channels(o_ref, scr, base):
    def channel(c, _):
        for n in range(COLS // LANES):
            o_ref[c, :, n * LANES:(n + 1) * LANES] = scr[pl.ds(base[n] + c, FB, stride=PITCH), :].astype(BF16)
        return 0

    lax.fori_loop(0, HID, channel, 0, unroll=16)


def bases(t):
    return [(t * (COLS // LANES) + n) * FB * PITCH for n in range(COLS // LANES)]


def column(row_ref):
    cols = row_ref[...].astype(F32).T
    return jnp.concatenate([cols[:, n:n + 1] for n in range(cols.shape[1])], axis=0)


def out_weights(gate_ref, gain_ref, proj_ref, gate_t, gain, proj_t):
    gate_t[...] = (gate_ref[...].astype(F32).T * 0.5).astype(BF16)
    gain[...] = column(gain_ref)
    proj_t[...] = (proj_ref[...].astype(F32).T * 0.5).astype(BF16)


def back_body(step, a0, a1, b0, b1, z_ref, x_ref, o_ref, gate_ref, gain_ref, proj_ref, o_scr):
    @pl.when(step < N_C)
    def _():
        for c in range(CB):
            dims = (((1,), (1,)), ((), ()))
            acc = lax.dot_general(a0[0, c], b0[0, c], dims, preferred_element_type=F32)
            acc = acc + lax.dot_general(a1[0, c], b1[0, c], dims, preferred_element_type=F32)
            o_scr[pl.ds(pl.multiple_of((step * CB + c) * OPITCH, 4), ROWS), :] = acc

    @pl.when(step >= N_C)
    def _():
        first = (step - N_C) * IB
        gain = gain_ref[...]

        def one_row(i, _):
            tri = o_scr[pl.ds(first + i, HID, stride=OPITCH), :]
            y = normed_t(tri, gain).astype(BF16)
            u = jnp.dot(proj_ref[...], y, preferred_element_type=F32)
            t = jnp.tanh(jnp.dot(gate_ref[...], x_ref[i], preferred_element_type=F32))
            z = z_ref[i].reshape(2 * HALF, PAIR).astype(F32)
            o_ref[i, :, o_ref.shape[2] - HALF:] = (z + (u + t * u).T).astype(BF16).reshape(2, HALF, PAIR)
            return 0

        lax.fori_loop(0, IB, one_row, 0, unroll=32)


def back_specs(half):
    def chan(slot):
        return pl.BlockSpec((1, CB, ROWS, COLS), lambda s: (slot, jnp.minimum(s, N_C - 1), 0, 0))

    tile = pl.BlockSpec((IB, 2, HALF, PAIR), lambda s: (jnp.maximum(s - N_C, 0), 0, half, 0))
    first = pl.BlockSpec((IB, 2, HALF, PAIR), lambda s: (jnp.maximum(s - N_C, 0), 0, 0, 0))
    x_spec = pl.BlockSpec((IB, PAIR, 2 * HALF), lambda s: (jnp.maximum(s - N_C, 0), 0, half))
    return [chan(0), chan(1), chan(2 + 2 * half), chan(3 + 2 * half), tile, x_spec], first


def main_kernel(z_ref, z4_ref, mask_in, gain_in, proj_a, gate_a, proj_b, gate_b, gate_in, gout_in, proj_in,
                xb, g_ref, xt, out_ref,
                mask_ref, w_ref, gate_ref, gout_ref, proj_ref, zbuf, xubuf, xmbuf, xin, obuf, scr, o_scr,
                zsem, xusem, xmsem, xsem, osem,
                y_s, p_s, q_s, s0_s, s1_s, y_r, p_r, q_r, s0_r, s1_r):
    row, col = lax.axis_index('row'), lax.axis_index('col')
    chip, core = row // 2, row % 2
    ydev = {'col': 1 - col}
    xdev = {'row': (1 - chip) * 2 + core}
    sdev = {'row': chip * 2 + 1 - core}
    diag = chip == col
    off = chip != col
    mine = 1 - diag.astype(jnp.int32)

    def part(k, slot, ch):
        return xb.at[k, slot, pl.ds(ch * FB, FB)]

    def rdma(src, dst, send, recv, dev):
        return pltpu.make_async_remote_copy(src_ref=src, dst_ref=dst, send_sem=send, recv_sem=recv,
                                            device_id=dev, device_id_type=MESH)

    def piece(k, slot, n):
        return xb.at[k, slot, pl.ds(LAST * FB + PIECES[n], PIECES[n + 1] - PIECES[n])]

    def p_piece(n):
        return rdma(piece(0, 0, n), piece(0, 1, n), p_s.at[LAST + n], p_r.at[LAST + n], xdev)

    def q_piece(n):
        return rdma(piece(1, 1, n), piece(1, 1, n), q_s.at[LAST + n], q_r.at[LAST + n], ydev)

    def s0_piece(n):
        return rdma(piece(0, mine, n), piece(0, 2, n), s0_s.at[LAST + n], s0_r.at[LAST + n], sdev)

    def s1_piece(n):
        return rdma(piece(1, mine, n), piece(1, 2, n), s1_s.at[LAST + n], s1_r.at[LAST + n], sdev)

    def y(ch):
        return rdma(part(0, 0, ch), part(1, 0, ch), y_s.at[ch], y_r.at[ch], ydev)

    def p(ch):
        return rdma(part(0, 0, ch), part(0, 1, ch), p_s.at[ch], p_r.at[ch], xdev)

    def q_relay(ch):
        return rdma(part(1, 0, ch), part(1, 1, ch), q_s.at[ch], q_r.at[ch], xdev)

    def q_hop(ch):
        return rdma(part(0, 0, ch), part(1, 1, ch), q_s.at[ch], q_r.at[ch], xdev)

    def q_hop2(ch):
        return rdma(part(1, 1, ch), part(1, 1, ch), q_s.at[ch], q_r.at[ch], ydev)

    def s0(ch):
        return rdma(part(0, mine, ch), part(0, 2, ch), s0_s.at[ch], s0_r.at[ch], sdev)

    def s1(ch):
        return rdma(part(1, mine, ch), part(1, 2, ch), s1_s.at[ch], s1_r.at[ch], sdev)

    barrier = pltpu.get_barrier_semaphore()
    for dev in (ydev, xdev, sdev):
        pl.semaphore_signal(barrier, inc=1, device_id=dev, device_id_type=MESH)

    def zload(ch):
        return pltpu.make_async_copy(z_ref.at[pl.ds(ch * FB, FB)], zbuf.at[ch % 2], zsem.at[ch % 2])

    def xustore(ch):
        return pltpu.make_async_copy(xubuf.at[ch % 2], xt.at[pl.ds(ch * FB, FB)], xusem.at[ch % 2])

    def xmstore(ch):
        return pltpu.make_async_copy(xmbuf.at[ch % 2], part(0, 0, ch), xmsem.at[ch % 2])

    def publish(ch):
        xmstore(ch).wait()
        y(ch).start()

        @pl.when(diag & (ch < LAST))
        def _():
            s0(ch).start()

        @pl.when(diag & (ch == LAST))
        def _():
            for n in range(N_P):
                s0_piece(n).start()

        @pl.when(diag & (ch < NH))
        def _():
            p(ch).start()

        @pl.when(off & (ch >= NH))
        def _():
            q_hop(ch).start()

    zload(0).start()
    gain = column(gain_in)
    mask = mask_in[...]
    mask_ref[...] = jnp.concatenate([mask[:, n * HALF:(n + 1) * HALF] for n in (0, 2, 1, 3)], axis=1)

    def norm_step(ch, _):
        @pl.when(ch + 1 < NCH)
        def _():
            zload(ch + 1).start()

        @pl.when(ch >= 2)
        def _():
            xustore(ch - 2).wait()

        zload(ch).wait()
        norm_chunk(zbuf.at[ch % 2], mask_ref, ch * FB, gain, xubuf.at[ch % 2], xmbuf.at[ch % 2])
        xustore(ch).start()
        xmstore(ch).start()

        @pl.when(ch == 0)
        def _():
            pl.semaphore_wait(barrier, 3)
            publish(0)

        @pl.when(ch >= 2)
        def _():
            publish(ch - 1)
        return 0

    lax.fori_loop(0, NCH, norm_step, 0)
    publish(NCH - 1)
    xustore(NCH - 2).wait()
    xustore(NCH - 1).wait()

    for n, (proj, gate) in enumerate(((proj_a, gate_a), (proj_b, gate_b))):
        for half, ref in ((0, proj), (1, gate)):
            w_t = (ref[...].astype(F32).T * 0.5).astype(BF16)
            for c in range(HID // CH):
                w_ref[n, pl.ds((2 * c + half) * CH, CH), :] = w_t[c * CH:(c + 1) * CH]
    out_weights(gate_in, gout_in, proj_in, gate_ref, gout_ref, proj_ref)

    def xload(k, slot, ch, t):
        return pltpu.make_async_copy(part(k, slot, ch), xin.at[t], xsem.at[t])

    def ostore(dst, block, t):
        return pltpu.make_async_copy(obuf.at[t % 2], g_ref.at[dst, :, pl.ds(block * FB, FB), :], osem.at[t % 2])

    def project(first_use, t, weight, dst, block):
        @pl.when(jnp.logical_not(first_use))
        def _():
            ostore(0, 0, t).wait()
        project_rows(xin.at[t], w_ref.at[weight], range(FB), scr, bases(0))
        write_channels(obuf.at[t % 2], scr, bases(0))
        ostore(dst, block, t).start()

    def window1(i, _):
        k, ch = i // NH, i % NH
        y(i).wait_recv()

        @pl.when(diag & (i < LAST))
        def _():
            s1(i).start()

        @pl.when(diag & (i == LAST))
        def _():
            for n in range(N_P):
                s1_piece(n).start()

        @pl.when(diag & (i < NH))
        def _():
            q_relay(i).start()

        @pl.when(diag & (i == NH - 1))
        def _():
            for c in range(NH, LAST):
                p(c).start()
            for n in range(N_P):
                p_piece(n).start()

        @pl.when(diag & (i >= NH))
        def _():
            q_hop(i).wait_recv()

        @pl.when(diag & (i >= NH) & (i < LAST))
        def _():
            q_hop2(i).start()

        @pl.when(diag & (i == LAST))
        def _():
            for n in range(N_P):
                q_piece(n).start()

        @pl.when(off & (i < NH))
        def _():
            p(ch).wait_recv()
            s0(ch).start()

        @pl.when(off & (i >= NH))
        def _():
            q_relay(ch).wait_recv()
            s1(ch).start()

        xload(0, 0, i, 0).start()
        xload(1, 0, i, 1).start()
        xload(k, mine, ch, 2).start()

        def step(t, _):
            @pl.when((t == 1) & (i < NH))
            def _():
                s0(ch).wait_recv()

            @pl.when((t == 1) & (i >= NH))
            def _():
                s1(ch).wait_recv()

            @pl.when(t == 1)
            def _():
                xload(k, 2, ch, 3).start()

            xload(0, 0, 0, t).wait()
            is_b = t // 2
            own_block = jnp.where(t == 2, core, 1 - core) * NH + ch
            project((i == 0) & (t < 2), t, is_b, jnp.where(is_b == 1, 2 + k, t), jnp.where(is_b == 1, own_block, i))
            return 0

        lax.fori_loop(0, 4, step, 0)
        return 0

    lax.fori_loop(0, NCH, window1, 0)
    ostore(0, 0, 0).wait()
    ostore(0, 0, 1).wait()

    specs, out_spec = back_specs(0)

    def pipe(a0, a1, b0, b1, zr, xr, o):
        back_body(pl.program_id(0), a0, a1, b0, b1, zr, xr, o, gate_ref, gout_ref, proj_ref, o_scr)

    pltpu.emit_pipeline(pipe, grid=(N_C + N_I,), in_specs=specs, out_specs=[out_spec])(
        g_ref, g_ref, g_ref, g_ref, z4_ref, xt, out_ref)

    def window2(i, _):
        ch = NH + i

        @pl.when(off)
        def _():
            p(ch).wait_recv()
            s0(ch).start()
            q_hop2(ch).wait_recv()
            s1(ch).start()

        xload(0, mine, ch, 0).start()
        xload(1, mine, ch, 1).start()

        def step(t, _):
            @pl.when(t == 1)
            def _():
                s0(ch).wait_recv()
                xload(0, 2, ch, 2).start()
                s1(ch).wait_recv()
                xload(1, 2, ch, 3).start()

            xload(0, 0, 0, t).wait()
            project((i == 0) & (t < 2), t, 1, 4 + t % 2, jnp.where(t < 2, core, 1 - core) * NH + i)
            return 0

        lax.fori_loop(0, 4, step, 0)
        return 0

    lax.fori_loop(0, LAST - NH, window2, 0)

    def xpiece(k, slot, n, t):
        return pltpu.make_async_copy(piece(k, slot, n), xin.at[t, pl.ds(PIECES[n], PIECES[n + 1] - PIECES[n])], xsem.at[t])

    for n in range(N_P):
        @pl.when(off)
        def _(n=n):
            p_piece(n).wait_recv()
            s0_piece(n).start()

        xpiece(0, mine, n, 0).start()

        @pl.when(off)
        def _(n=n):
            q_piece(n).wait_recv()
            s1_piece(n).start()

        xpiece(1, mine, n, 1).start()
        for t in range(4):
            if t == 1:
                s0_piece(n).wait_recv()
                xpiece(0, 2, n, 2).start()
                s1_piece(n).wait_recv()
                xpiece(1, 2, n, 3).start()
            xpiece(0, 0, n, t).wait()
            project_rows(xin.at[t], w_ref.at[1], range(PIECES[n], PIECES[n + 1]), o_scr, bases(t))
            if n == N_P - 1:
                ostore(0, 0, t).wait()
                write_channels(obuf.at[t % 2], o_scr, bases(t))
                ostore(4 + t % 2, (core if t < 2 else 1 - core) * NH + LAST - NH, t).start()
    ostore(0, 0, 0).wait()
    ostore(0, 0, 1).wait()

    def drain(ch, _):
        y(ch).wait_send()

        @pl.when(ch < LAST)
        def _():
            s0(ch).wait_send()
            s1(ch).wait_send()

        @pl.when(diag & (ch < LAST))
        def _():
            p(ch).wait_send()

        @pl.when((diag & (ch < LAST)) | (off & (ch >= NH)))
        def _():
            q_hop(ch).wait_send()
        return 0

    lax.fori_loop(0, NCH, drain, 0)
    for n in range(N_P):
        s0_piece(n).wait_send()
        s1_piece(n).wait_send()

        @pl.when(diag)
        def _(n=n):
            p_piece(n).wait_send()
            q_piece(n).wait_send()


def last_back_kernel(a0, a1, b0, b1, z_ref, x_ref, gate_ref, gain_ref, proj_ref, first_ref, o_ref, gate_t, gain, proj_t, o_scr):
    step = pl.program_id(0)

    @pl.when(step == 0)
    def _():
        out_weights(gate_ref, gain_ref, proj_ref, gate_t, gain, proj_t)

    @pl.when(step >= N_C)
    def _():
        o_ref[:, :, :HALF] = first_ref[...]
    back_body(step, a0, a1, b0, b1, z_ref, x_ref, o_ref, gate_t, gain, proj_t, o_scr)


def solution(mesh):
    tile_spec = P(('batch', 'row'), 'col', None)
    mask_spec = P(('batch', 'row'), 'col')
    repl_spec = P()
    any_spec = pl.BlockSpec(memory_space=pl.ANY)
    vmem_spec = pl.BlockSpec(memory_space=pltpu.VMEM)
    dma = pltpu.SemaphoreType.DMA

    def per_device(z_tile, mask_tile, ln_in_gain, proj_a, gate_a, proj_b, gate_b, gate_out, proj_out, ln_out_gain):
        gain_in, gain_out = ln_in_gain.reshape(1, PAIR), ln_out_gain.reshape(HID // LANES, LANES)
        z4 = z_tile.reshape(ROWS, 2, 2 * HALF, PAIR)
        out_w = [pltpu.VMEM((PAIR, PAIR), BF16), pltpu.VMEM((HID, 1), F32), pltpu.VMEM((PAIR, HID), BF16)]

        _, g, xt, first = pl.pallas_call(
            main_kernel,
            out_shape=(
                jax.ShapeDtypeStruct((2, 3, ROWS, PAIR, COLS), BF16),
                jax.ShapeDtypeStruct((6, HID, ROWS, COLS), BF16),
                jax.ShapeDtypeStruct((ROWS, PAIR, COLS), BF16),
                jax.ShapeDtypeStruct((ROWS, 2, HALF, PAIR), BF16),
            ),
            in_specs=[any_spec, any_spec] + [vmem_spec] * 9,
            out_specs=(any_spec,) * 4,
            scratch_shapes=[
                pltpu.VMEM((ROWS, COLS), jnp.int32),
                pltpu.VMEM((2, 2 * HID, PAIR), BF16),
                *out_w,
                pltpu.VMEM((2, FB, COLS, PAIR), BF16),
                pltpu.VMEM((2, FB, PAIR, COLS), BF16),
                pltpu.VMEM((2, FB, PAIR, COLS), BF16),
                pltpu.VMEM((4, FB, PAIR, COLS), BF16),
                pltpu.VMEM((2, HID, FB, COLS), BF16),
                pltpu.VMEM((COLS // LANES * FB * PITCH, LANES), F32),
                pltpu.VMEM((HID * OPITCH, 2 * HALF), F32),
                dma((2,)), dma((2,)), dma((2,)), dma((4,)), dma((2,)),
            ] + [dma((LAST + N_P,))] * 10,
            compiler_params=pltpu.CompilerParams(vmem_limit_bytes=VMEM_LIMIT, collective_id=0, has_side_effects=True),
            name='exchange_project',
        )(z_tile, z4, mask_tile, gain_in, proj_a, gate_a, proj_b, gate_b, gate_out, gain_out, proj_out)

        def whole(*shape):
            return pl.BlockSpec(shape, lambda s: (0,) * len(shape))

        specs, first_spec = back_specs(1)
        out = pl.pallas_call(
            last_back_kernel,
            grid=(N_C + N_I,),
            out_shape=jax.ShapeDtypeStruct((ROWS, 2, 2 * HALF, PAIR), BF16),
            in_specs=specs + [whole(PAIR, PAIR), whole(HID // LANES, LANES), whole(HID, PAIR), first_spec],
            out_specs=pl.BlockSpec((IB, 2, 2 * HALF, PAIR), lambda s: (jnp.maximum(s - N_C, 0), 0, 0, 0)),
            scratch_shapes=[*out_w, pltpu.VMEM((HID * OPITCH, 2 * HALF), F32)],
            compiler_params=pltpu.CompilerParams(vmem_limit_bytes=VMEM_LIMIT),
            name='back',
        )(g, g, g, g, z4, xt, gate_out, gain_out, proj_out, first)
        return out.reshape(ROWS, COLS, PAIR)

    return jax.shard_map(per_device, mesh=mesh, in_specs=(tile_spec, mask_spec) + (repl_spec,) * 8, out_specs=tile_spec, check_vma=False)
```
